256 devices in a mesh: site: 2 (over y), pts: 128 (over z, x, core).
Axes of the slice: x: 4, y: 2, z: 16, core: 2. Of those that a mesh axis runs over, the one named last changes fastest.
The devices are a block of a 4x16x16 slice.
Arguments:
- green_tensors: bfloat16 [4096, 4, 6, 2, 1024], P(('site', 'pts')), parts along dimension 0, may hold values from -6 to 6
- block_lists: int32 [256, 32], P(('site', 'pts')), parts along dimension 0, may hold values from 0 to 2047, as said below
- block_count: int32 [256], P(('site', 'pts')), parts along dimension 0, may hold values from 1 to 32
- onset_steps: int32 [256, 16, 128], P(('site', 'pts')), parts along dimension 0, may hold values from 0 to 255
- slip_amount: float32 [256, 16, 128], P(('site', 'pts')), parts along dimension 0, may hold values from 0.2 to 2
- mechanism: float32 [256, 6], P(('site', 'pts')), parts along dimension 0, may hold values from -2.4 to 2.4
- slip_rate: float32 [256, 16, 128], P(('site', 'pts')), parts along dimension 0, may hold values from 0.005 to 0.05
Outputs:
- seismograms: float32 [256, 16, 2, 1024], P(('site', 'pts')), parts along dimension 0
The draws below stay inside these ranges and needn't reach their ends.
There are 2 independent parts, one for each index of `site`. The reference program is written for one: setup_inputs(seed, part) draws one part's arguments, and reference() takes and returns one part's arrays. A program takes and returns all parts, laid end to end along the dimension named above; each array names one. Nothing has to cross between parts.
Inputs may be any that keep to these rules, and one draw needn't show every extreme that they name: `block_lists`: numbers of point blocks; the ruptures held by one device name at most 1 entries in blocks held by any one device, and exactly 1 for some holder.
All inputs are finite; a program needn't handle non-finite values.
Results may differ from the reference program's by a relative error of at most 0.0003.
Values may be sent and summed in bfloat16 or wider, within the bound.
A program may use at most 128 MiB of HBM per device.

```python
import math
import jax
import jax.numpy as jnp
from jax import lax

NT = 1024
P_SIZE = 4
K = 32
V = 16
L = 128
MAXON = 256
BD = 16
RD = 1
NB = 2048
R = 128
N_PTS = 128


def draw_block_lists(key, part):
    entries = RD * K

    def per_worker(worker):
        worker_key = jax.random.fold_in(jax.random.fold_in(key, 11), worker)
        holders = jax.random.permutation(worker_key, N_PTS)
        order = jnp.arange(entries, dtype=jnp.int32)
        holder_of = holders[order % N_PTS]
        local_block = jax.random.randint(jax.random.fold_in(worker_key, 1), (entries,), 0, BD)
        return (holder_of * BD + local_block).astype(jnp.int32)
    lists = jax.vmap(per_worker)(jnp.arange(N_PTS, dtype=jnp.int32))
    return lists.reshape(RD * N_PTS, K)


def set_ends(values, own_key, low, top_value):
    index_at = [jax.random.randint(jax.random.fold_in(own_key, axis), (), 0, length) for axis, length in enumerate(values.shape)]
    main_axis = values.shape.index(max(values.shape))
    beside = index_at[:main_axis] + [(index_at[main_axis] + 1) % values.shape[main_axis]] + index_at[main_axis + 1:]
    return values.at[tuple(index_at)].set(low).at[tuple(beside)].set(top_value)


def steps_of(own_key, dims, cuts, smallest, top_value):
    def one(dim, blocks):
        draws = jax.random.uniform(jax.random.fold_in(jax.random.fold_in(own_key, 6), dim), (blocks,), jnp.float32, smallest / len(cuts), top_value / len(cuts))
        return jnp.repeat(jnp.exp(draws), dims[dim] // blocks).reshape((-1,) + (1,) * (len(dims) - dim - 1))

    gain = one(*cuts[0])
    for cut in cuts[1:]:
        gain = gain * one(*cut)
    return gain


def normal_values(rng, shape, scale, limit, cuts=(), kind=jnp.bfloat16):
    array = scale * jax.random.normal(rng, shape, jnp.float32)
    if cuts:
        array = array * steps_of(rng, shape, cuts, -0.22, 0.18)
    return jnp.clip(array, -limit, limit).astype(kind)


def setup_inputs(seed: int = 0, part: int = 0) -> dict:
    keys = jax.random.split(jax.random.key(seed), 8)
    part_keys = jax.random.split(jax.random.fold_in(keys[7], part), 8)
    return {
        "green_tensors": normal_values(part_keys[0], (NB, P_SIZE, 6, 2, NT), 1.0, 6.0, ((0, 128),)),
        "block_lists": draw_block_lists(jax.random.fold_in(jax.random.fold_in(keys[7], part), 71), part),
        "block_count": set_ends(jax.random.randint(part_keys[2], (R,), 1, K + 1), jax.random.fold_in(part_keys[2], 1), 1, K).astype(jnp.int32),
        "onset_steps": set_ends(jax.random.randint(part_keys[3], (R, V, K * P_SIZE), 0, MAXON), jax.random.fold_in(part_keys[3], 1), 0, MAXON - 1).astype(jnp.int32),
        "slip_amount": jnp.clip(jnp.exp(math.log(2.0) - 2.3025851 * jax.random.uniform(part_keys[4], (R, V, K * P_SIZE), jnp.float32) ** steps_of(part_keys[4], (R, V, K * P_SIZE), ((0, 128),), -0.2, 0.2)), 0.2, 2.0),
        "mechanism": normal_values(part_keys[5], (R, 6), 0.4, 2.4, ((0, 128),), jnp.float32),
        "slip_rate": jnp.clip(jnp.exp(math.log(0.05) - 2.3025851 * jax.random.uniform(part_keys[6], (R, V, L), jnp.float32) ** steps_of(part_keys[6], (R, V, L), ((0, 128),), -0.2, 0.2)), 0.005, 0.05),
    }


def lag_traces(traces, onsets):
    steps = jnp.arange(traces.shape[-1], dtype=jnp.int32)
    source = steps[None, :] - onsets[:, None]
    inside = source >= 0
    picked = jnp.take_along_axis(traces, jnp.broadcast_to(jnp.maximum(source, 0)[:, None, :], traces.shape), axis=2)
    return jnp.where(inside[:, None, :], picked, 0.0)


def weighted_sum(traces, weights, onsets):
    def per_variation(weight_row, onset_row):
        return jnp.sum(weight_row[:, None, None] * lag_traces(traces, onset_row), axis=0)
    return jax.vmap(per_variation)(weights, onsets)


def reference(green_tensors, block_lists, block_count, onset_steps, slip_amount, mechanism, slip_rate):
    listed = block_lists.shape[1]
    length = green_tensors.shape[-1]

    def per_rupture(inputs):
        blocks, listed_count, onset_rows, slip_rows, mech_row, rate_rows = inputs
        chosen = jnp.take(green_tensors, blocks, axis=0).astype(jnp.float32)
        traces = jnp.einsum("kpsct,s->kpct", chosen, mech_row, precision=lax.Precision.HIGHEST)
        kept_mask = (jnp.arange(listed, dtype=jnp.int32) < listed_count).astype(jnp.float32)
        points = chosen.shape[1]
        weights = slip_rows * jnp.repeat(kept_mask, points)[None, :]
        motion = weighted_sum(traces.reshape(-1, 2, length), weights, onset_rows)

        def convolve_row(signal, kernel):
            return jnp.convolve(signal, kernel, precision=lax.Precision.HIGHEST)[:length]

        return jax.vmap(jax.vmap(convolve_row, (0, None)), (0, 0))(motion, rate_rows)

    return lax.map(per_rupture, (block_lists, block_count, onset_steps, slip_amount, mechanism, slip_rate))
```

```python
import functools

import jax
import jax.numpy as jnp
import numpy as np
from jax import lax
from jax.experimental import pallas as pl
from jax.experimental.pallas import tpu as pltpu
from jax.sharding import PartitionSpec as P

MESH = pl.DeviceIdType.MESH
HIGHEST = lax.Precision.HIGHEST
SITE_PTS = ("site", "pts")
PLANE = 8
LIMIT = 6.0
TOP = 32767.0
CHUNK = 4
BLOCKS = 16
VMEM_LIMIT = 60 * 1024 * 1024


def mate(j, e):
    for bit in (1, 2, 4):
        if e & bit:
            j = j + bit * (1 - 2 * ((j // bit) % 2))
    return j


def partner(index):
    return {"pts": index}


def train_of(planes):
    half = planes // 2
    dz = np.arange(planes * PLANE) // PLANE
    e = np.arange(planes * PLANE) % PLANE
    up = ((dz >= 1) & (dz < half)) | ((dz == half) & (e < PLANE // 2))
    down = (dz > half) | ((dz == half) & (e >= PLANE // 2))
    distance = np.where(up, dz, np.where(down, planes - dz, 0))
    return distance, up.astype(np.int32) - down.astype(np.int32), e


def before_table(planes):
    distance, way, e = train_of(planes)
    same = (way[:, None] == way[None, :]) & (way[:, None] != 0)
    ahead = (distance[:, None] > distance[None, :]) | (
        (distance[:, None] == distance[None, :]) & (e[:, None] < e[None, :])
    )
    return (same & ahead).astype(np.float32)


def reach_tables(planes, caps):
    distance, way, e = train_of(planes)
    half = planes // 2
    size = planes * PLANE
    reach = np.zeros((size, size), np.float32)
    limit = np.full((4 * planes, size), 1e6, np.float32)
    for chip in range(4):
        turned = np.arange(size) ^ (2 * chip)
        for s in range(1, half + 1):
            for w, sign in enumerate((1, -1)):
                column = chip * planes + w * half + s - 1
                reach[:, column] = ((way == sign) & (distance >= s))[turned]
                limit[chip * planes : (chip + 1) * planes, column] = caps[s - 1]
    return reach, limit


def most_packets(planes):
    half = planes // 2
    return tuple(2 * (PLANE * (half - s) + PLANE // 2) for s in range(1, half + 1))


def exchange_kernel(
    planes, list_ref, count_ref, moment_ref, before_ref, reach_ref, limit_ref, green_ref,
    tab_ref, block_ref, place_ref, over_ref, other_ref,
    row_ref, rows_ref, send_a, recv_a, send_b, recv_b, send_g, recv_g,
):
    me = lax.axis_index("pts")
    z, j = me // PLANE, me % PLANE
    size = planes * PLANE
    listed = list_ref.shape[1]
    strains = moment_ref.shape[1]

    barrier = pltpu.get_barrier_semaphore()
    for e in range(1, PLANE):
        pl.semaphore_signal(
            barrier, inc=1, device_id=partner(z * PLANE + mate(j, e)), device_id_type=MESH
        )
    for d in range(1, planes):
        pl.semaphore_signal(
            barrier, inc=1, device_id=partner(((z + d) % planes) * PLANE + j), device_id_type=MESH
        )
    entry = lax.broadcasted_iota(jnp.int32, (1, listed), 1)
    names = jnp.where(entry < count_ref[0], list_ref[...], -1).astype(jnp.float32)
    row_ref[...] = jnp.zeros_like(row_ref)
    row_ref[0, :, pl.ds(0, listed)] = names
    row_ref[0, :, pl.ds(listed + 1, strains)] = moment_ref[...]
    rows_ref[pl.ds(0, 1)] = row_ref[...]
    pl.semaphore_wait(barrier, PLANE - 1 + planes - 1)

    copies = []
    for e in range(1, PLANE):
        copies.append(
            pltpu.make_async_remote_copy(
                src_ref=row_ref,
                dst_ref=rows_ref.at[pl.ds(e, 1)],
                send_sem=send_a.at[e],
                recv_sem=recv_a.at[e],
                device_id=partner(z * PLANE + mate(j, e)),
                device_id_type=MESH,
            )
        )
    for copy in copies:
        copy.start()
    green = pltpu.make_async_remote_copy(
        src_ref=green_ref,
        dst_ref=other_ref,
        send_sem=send_g,
        recv_sem=recv_g,
        device_id=partner(z * PLANE + mate(j, 1)),
        device_id_type=MESH,
    )
    green.start()
    for copy in copies:
        copy.wait()
    copies = []
    for d in range(1, planes):
        copies.append(
            pltpu.make_async_remote_copy(
                src_ref=rows_ref.at[pl.ds(0, PLANE)],
                dst_ref=rows_ref.at[pl.ds((planes - d) * PLANE, PLANE)],
                send_sem=send_b.at[d],
                recv_sem=recv_b.at[d],
                device_id=partner(((z + d) % planes) * PLANE + j),
                device_id_type=MESH,
            )
        )
    for copy in copies:
        copy.start()
    for copy in copies:
        copy.wait()

    turned = rows_ref[...].reshape(size, 128).T
    named = turned[:listed]
    holder = jnp.floor(named * (1.0 / BLOCKS))
    source = lax.broadcasted_iota(jnp.int32, (size, size), 0)
    lane = lax.broadcasted_iota(jnp.int32, (size, size), 1)
    at = (z + planes - (source & (planes - 1))) & (planes - 1)
    source_id = (at * PLANE + (j ^ (source // planes))).astype(jnp.float32)
    active = jnp.zeros((size, size), jnp.float32)
    for k in range(listed):
        active = active + jnp.where(holder[k : k + 1, :] == source_id, 1.0, 0.0)
    view = pltpu.roll(active, 0, 1, stride=PLANE, stride_axis=0)
    chips = jnp.concatenate(
        [
            view[2 * g * planes : (2 * g + 1) * planes] + view[(2 * g + 1) * planes : (2 * g + 2) * planes]
            for g in range(4)
        ],
        axis=0,
    ).astype(jnp.bfloat16)
    counts = jnp.dot(chips, reach_ref[...], preferred_element_type=jnp.float32)
    excess = jnp.max(counts - limit_ref[...], axis=0, keepdims=True)
    excess = jnp.max(excess, axis=1, keepdims=True)
    over_ref[...] = jnp.broadcast_to(jnp.where(excess > 0.5, 1, 0), (8, 128)).astype(jnp.int32)

    first = jnp.dot(chips[:planes], before_ref[...], preferred_element_type=jnp.float32)
    second = first + view[:planes]
    diagonal = (lane[:planes] // PLANE) == source[:planes]
    part = lax.broadcasted_iota(jnp.int32, (8, size), 0)
    place = jnp.where(
        part == 0,
        jnp.sum(jnp.where(diagonal, first, 0.0), axis=0, keepdims=True),
        jnp.sum(jnp.where(diagonal, second, 0.0), axis=0, keepdims=True),
    )
    place_ref[...] = place.astype(jnp.int32)

    moment = turned[32:40]
    bound = LIMIT * jnp.sum(
        jnp.where((part >= 1) & (part <= strains), jnp.abs(moment), 0.0), axis=0, keepdims=True
    )
    gain = 1.0 / jnp.maximum(bound, 1e-30)
    moment = jnp.where(part == 7, gain, moment)
    side = lane[:1]
    way = jnp.where(side < PLANE, 0, jnp.where(side < (planes // 2) * PLANE + PLANE // 2, 1, -1))
    mine = way == 1 - 2 * (j % 2)
    slot = source.astype(jnp.float32)

    def info(owner, shift):
        owner = owner.astype(jnp.float32)
        block = jnp.where(holder == owner, named - (BLOCKS * owner - shift), 0.0)
        return jnp.where(part == 0, jnp.sum(block, axis=0, keepdims=True), moment)

    def table(which, held, position):
        chosen = (held > 0.5) & mine & (position == slot)
        return lax.dot_general(
            which,
            jnp.where(chosen, 1.0, 0.0),
            (((1,), (1,)), ((), ())),
            precision=HIGHEST,
            preferred_element_type=jnp.float32,
        )

    own = info(me, 0.0)
    both = table(own, view[:1], first[:1]) + table(
        info(me + 1 - 2 * (j % 2), float(BLOCKS)), view[planes : planes + 1], second[:1]
    )
    tab_ref[:, :size] = both
    tab_ref[:, size:] = own
    block_ref[:, :size] = both.astype(jnp.int32)
    block_ref[:, size:] = own.astype(jnp.int32)
    green.wait()


def exchange(planes, caps, lists, count, moment, green):
    size = planes * PLANE
    before = before_table(planes)
    reach, limit = reach_tables(planes, caps)
    vmem = pl.BlockSpec(memory_space=pltpu.VMEM)
    smem = pl.BlockSpec(memory_space=pltpu.SMEM)
    hbm = pl.BlockSpec(memory_space=pl.ANY)
    return pl.pallas_call(
        functools.partial(exchange_kernel, planes),
        out_shape=(
            jax.ShapeDtypeStruct((8, 2 * size), jnp.float32),
            jax.ShapeDtypeStruct((8, 2 * size), jnp.int32),
            jax.ShapeDtypeStruct((8, size), jnp.int32),
            jax.ShapeDtypeStruct((8, 128), jnp.int32),
            jax.ShapeDtypeStruct(green.shape, green.dtype),
        ),
        in_specs=[vmem, smem, vmem, vmem, vmem, vmem, hbm],
        out_specs=(vmem, vmem, vmem, vmem, hbm),
        scratch_shapes=[
            pltpu.VMEM((1, 1, 128), jnp.float32),
            pltpu.VMEM((size, 1, 128), jnp.float32),
            pltpu.SemaphoreType.DMA((PLANE,)),
            pltpu.SemaphoreType.DMA((PLANE,)),
            pltpu.SemaphoreType.DMA((planes,)),
            pltpu.SemaphoreType.DMA((planes,)),
            pltpu.SemaphoreType.DMA,
            pltpu.SemaphoreType.DMA,
        ],
        compiler_params=pltpu.CompilerParams(collective_id=0, has_side_effects=True),
        name="exchange",
    )(
        lists, count, moment, jnp.asarray(before, jnp.bfloat16), jnp.asarray(reach, jnp.bfloat16),
        jnp.asarray(limit), green,
    )


def spans(count):
    return [(first, min(first + CHUNK, count)) for first in range(0, count, CHUNK)]


def carry_kernel(planes, caps, place_ref, block_ref, tab_ref, mine_ref, other_ref, out_ref, *scratch):
    half = planes // 2
    green, own, staged, near = scratch[:4]
    moved = scratch[4 : 4 + half]
    load, send_z, recv_z, send_x, recv_x, send_n, recv_n = scratch[4 + half :]
    me = lax.axis_index("pts")
    z, j = me // PLANE, me % PLANE
    w = j % 2
    size = planes * PLANE

    loads = [
        pltpu.make_async_copy(mine_ref, green.at[pl.ds(0, BLOCKS)], load.at[0]),
        pltpu.make_async_copy(other_ref, green.at[pl.ds(BLOCKS, BLOCKS)], load.at[1]),
    ]
    for copy in loads:
        copy.start()
    barrier = pltpu.get_barrier_semaphore()
    for e in range(1, PLANE):
        pl.semaphore_signal(
            barrier, inc=1, device_id=partner(z * PLANE + mate(j, e)), device_id_type=MESH
        )
    for way in (1, planes - 1):
        pl.semaphore_signal(
            barrier, inc=1, device_id=partner(((z + way) % planes) * PLANE + j), device_id_type=MESH
        )
    for copy in loads:
        copy.wait()
    pl.semaphore_wait(barrier, PLANE - 1 + 2)

    def trace(entry, write):
        block = jnp.clip(block_ref[0, entry], 0, 2 * BLOCKS - 1)
        moment = [tab_ref[1 + s, entry] for s in range(6)]
        gain = tab_ref[7, entry]
        for p in range(4):
            total = moment[0] * green[block, p, 0].astype(jnp.float32)
            for s in range(1, 6):
                total = total + moment[s] * green[block, p, s].astype(jnp.float32)
            root = lax.rsqrt(lax.rsqrt(jnp.abs(total) * gain))
            level = jnp.minimum(root * TOP, TOP)
            code = jnp.round(jnp.where(total < 0.0, -level, level)).astype(jnp.int32)
            write(p, code.astype(jnp.int16))

    def hop(s, c):
        first, last = spans(caps[s])[c]
        source = own if s == 0 else moved[s - 1]
        return pltpu.make_async_remote_copy(
            src_ref=source.at[pl.ds(first, last - first)],
            dst_ref=moved[s].at[pl.ds(first, last - first)],
            send_sem=send_z.at[s, c],
            recv_sem=recv_z.at[s, c],
            device_id=partner(((z + 1 + w * (planes - 2)) % planes) * PLANE + j),
            device_id_type=MESH,
        )

    def offset(s):
        return (s + 1) + w * (planes - 2 * (s + 1))

    def spread(s, e):
        return pltpu.make_async_remote_copy(
            src_ref=staged.at[s, e],
            dst_ref=out_ref.at[offset(s), pl.ds(e - e % 2, 2)],
            send_sem=send_x.at[s, e],
            recv_sem=recv_x.at[offset(s), e // 2],
            device_id=partner(z * PLANE + mate(j, e)),
            device_id_type=MESH,
        )

    def visit(e):
        return pltpu.make_async_remote_copy(
            src_ref=near.at[e],
            dst_ref=out_ref.at[0, e],
            send_sem=send_n.at[e],
            recv_sem=recv_n.at[e],
            device_id=partner(z * PLANE + mate(j, e)),
            device_id_type=MESH,
        )

    for c, (first, last) in enumerate(spans(caps[0])):

        def fill(i, carry):
            def write(p, code):
                own[i, pl.ds(16 * p, 16), :] = code

            trace(i, write)
            return carry

        lax.fori_loop(first, last, fill, 0)
        hop(0, c).start()

    def write_own(p, code):
        out_ref[0, 0, pl.ds(16 * p, 16), :] = code

    trace(size, write_own)

    def fill_near(e, carry):
        def write(p, code):
            near[e, pl.ds(16 * p, 16), :] = code

        trace(size + e, write)
        return carry

    lax.fori_loop(1, PLANE, fill_near, 0)
    for e in range(1, PLANE):
        visit(e).start()

    def deliver(s, mates):
        q = offset(s)
        for e in mates:
            for r in range(2):
                at = jnp.clip(place_ref[r, q * PLANE + e], 0, caps[s] - 1)
                packet = moved[s][at]
                if e == 0:
                    out_ref[q, r] = packet
                else:
                    staged[s, e, (e + r) % 2] = packet
        for e in mates:
            if e:
                spread(s, e).start()

    low, high = range(PLANE // 2), range(PLANE // 2, PLANE)
    for s in range(half):
        for c, (first, last) in enumerate(spans(caps[s])):
            hop(s, c).wait_recv()
            if s + 1 < half and first < caps[s + 1]:
                hop(s + 1, c).start()
        if s + 1 < half:
            deliver(s, range(PLANE))
        else:

            @pl.when(w == 0)
            def _():
                deliver(half - 1, low)

            @pl.when(w == 1)
            def _():
                deliver(half - 1, high)

    for s in range(half):
        for c in range(len(spans(caps[s]))):
            hop(s, c).wait_send()
    for e in range(1, PLANE):
        visit(e).wait()
        for s in range(half - 1):
            spread(s, e).wait_send()

    @pl.when(w == 0)
    def _():
        for e in low:
            if e:
                spread(half - 1, e).wait_send()

    @pl.when(w == 1)
    def _():
        for e in high:
            spread(half - 1, e).wait_send()

    def arrival(q, chip):
        return pltpu.make_async_remote_copy(
            src_ref=staged.at[0, 1],
            dst_ref=out_ref.at[q, pl.ds(2 * chip, 2)],
            send_sem=send_x.at[0, 1],
            recv_sem=recv_x.at[q, chip],
            device_id=partner(z * PLANE + mate(j, 1)),
            device_id_type=MESH,
        )

    for q in range(1, planes):
        for chip in range(1, 4):
            arrival(q, chip).wait_recv()

    @pl.when(w == 1)
    def _():
        for q in range(1, half + 1):
            arrival(q, 0).wait_recv()

    @pl.when(w == 0)
    def _():
        for q in range(half + 1, planes):
            arrival(q, 0).wait_recv()


def carry(planes, caps, number, place, block, tab, mine, other):
    half = planes // 2
    chunks = len(spans(caps[0]))
    smem = pl.BlockSpec(memory_space=pltpu.SMEM)
    hbm = pl.BlockSpec(memory_space=pl.ANY)
    packet = (64, 128)
    return pl.pallas_call(
        functools.partial(carry_kernel, planes, caps),
        out_shape=jax.ShapeDtypeStruct((planes, PLANE, *packet), jnp.int16),
        in_specs=[smem, smem, smem, hbm, hbm],
        out_specs=pl.BlockSpec(memory_space=pltpu.VMEM),
        scratch_shapes=[
            pltpu.VMEM((2 * mine.shape[0], *mine.shape[1:]), mine.dtype),
            pltpu.VMEM((caps[0], *packet), jnp.int16),
            pltpu.VMEM((half, PLANE, 2, *packet), jnp.int16),
            pltpu.VMEM((PLANE, *packet), jnp.int16),
            *[pltpu.VMEM((caps[s], *packet), jnp.int16) for s in range(half)],
            pltpu.SemaphoreType.DMA((2,)),
            pltpu.SemaphoreType.DMA((half, chunks)),
            pltpu.SemaphoreType.DMA((half, chunks)),
            pltpu.SemaphoreType.DMA((half, PLANE)),
            pltpu.SemaphoreType.DMA((planes, 4)),
            pltpu.SemaphoreType.DMA((PLANE,)),
            pltpu.SemaphoreType.DMA((PLANE,)),
        ],
        compiler_params=pltpu.CompilerParams(
            collective_id=number, has_side_effects=True, vmem_limit_bytes=VMEM_LIMIT
        ),
        name="carry",
    )(place, block, tab, mine, other)


def halves(value):
    coarse = value.astype(jnp.bfloat16)
    return coarse, (value - coarse.astype(jnp.float32)).astype(jnp.bfloat16)


def motion_kernel(
    planes, list_ref, count_ref, onset_ref, slip_ref, moment_ref, packet_ref, rate_ref, out_ref,
    wide, motion,
):
    me = lax.axis_index("pts")
    z, j = me // PLANE, me % PLANE
    variations = out_ref.shape[0]
    bound = jnp.abs(moment_ref[0, 0])
    for s in range(1, 6):
        bound = bound + jnp.abs(moment_ref[0, s])
    unit = bound * (LIMIT / TOP**4)
    lane = lax.broadcasted_iota(jnp.int32, (16, 128), 1)
    motion[...] = jnp.zeros_like(motion)
    wide[...] = jnp.zeros_like(wide)

    def add_block(k, carry):
        holder = list_ref[0, k] // 16
        hz, hj = holder // PLANE, holder % PLANE
        q = (z - hz + planes) % planes
        e = j ^ hj
        for p in range(4):
            code = packet_ref[q, e, pl.ds(16 * p, 16), :].astype(jnp.int32).astype(jnp.float32)
            square = code * jnp.abs(code)
            wide[p, pl.ds(8, 16), :] = square * jnp.abs(square) * unit
        for v in range(variations):
            total = None
            for p in range(4):
                onset = onset_ref[v, k * 4 + p]
                whole = onset >> 7
                rest = onset & 127
                near = wide[p, pl.ds(8 - 2 * whole, 16), :]
                far = wide[p, pl.ds(6 - 2 * whole, 16), :]
                moved = pltpu.roll(jnp.where(lane < 128 - rest, near, far), rest, 1)
                term = slip_ref[v, k * 4 + p] * moved
                total = term if total is None else total + term
            motion[v, pl.ds(8, 16), :] += total
        return carry

    lax.fori_loop(0, count_ref[0], add_block, 0)

    row = lax.broadcasted_iota(jnp.int32, (128, 128), 0)
    column = lax.broadcasted_iota(jnp.int32, (128, 128), 1)
    for v in range(variations):
        rate = jnp.broadcast_to(rate_ref[pl.ds(v, 1), :], (128, 128))
        rate = pltpu.roll(rate, 0, 1, stride=1, stride_axis=0)
        taps = jnp.concatenate(
            [jnp.where(column >= row, rate, 0.0), jnp.where(column < row, rate, 0.0)], axis=0
        )
        signal = jnp.concatenate([motion[v, pl.ds(8, 16), :], motion[v, pl.ds(6, 16), :]], axis=1)
        coarse, fine = halves(signal)
        taps, rest = halves(taps)
        both = jnp.dot(
            jnp.concatenate([coarse, fine], axis=0), taps, preferred_element_type=jnp.float32
        )
        out_ref[v] = (
            both[:16] + both[16:] + jnp.dot(coarse, rest, preferred_element_type=jnp.float32)
        )


def synthesize(planes, block_list, count, onset, slip, moment, packets, rate):
    variations = onset.shape[0]
    smem = pl.BlockSpec(memory_space=pltpu.SMEM)
    vmem = pl.BlockSpec(memory_space=pltpu.VMEM)
    return pl.pallas_call(
        functools.partial(motion_kernel, planes),
        out_shape=jax.ShapeDtypeStruct((variations, 16, 128), jnp.float32),
        in_specs=[smem, smem, smem, smem, smem, vmem, vmem],
        out_specs=vmem,
        scratch_shapes=[
            pltpu.VMEM((4, 24, 128), jnp.float32),
            pltpu.VMEM((variations, 24, 128), jnp.float32),
        ],
        compiler_params=pltpu.CompilerParams(vmem_limit_bytes=VMEM_LIMIT),
        name="synthesize",
    )(block_list, count, onset, slip, moment, packets, rate)


CAPS = (37, 34, 30, 27, 23, 19, 14, 7)


def local(planes, green_tensors, block_lists, block_count, onset_steps, slip_amount, mechanism, slip_rate):
    held, points, strains, parts, length = green_tensors.shape
    green = green_tensors.reshape(held, points, strains, parts, length // 128, 128)
    green = green.transpose(0, 1, 2, 4, 3, 5).reshape(held, points, strains, -1, 128)
    tab, block, place, over, other = exchange(
        planes, CAPS, block_lists, block_count, mechanism, green
    )
    packets = lax.cond(
        over[0, 0] > 0,
        functools.partial(carry, planes, most_packets(planes), 1),
        functools.partial(carry, planes, CAPS, 2),
        place,
        block,
        tab,
        green,
        other,
    )
    seis = synthesize(
        planes, block_lists, block_count, onset_steps[0], slip_amount[0], mechanism, packets, slip_rate[0]
    )
    seis = seis.reshape(-1, length // 128, parts, 128).transpose(0, 2, 1, 3)
    return seis.reshape(1, -1, parts, length)


def solution(mesh):
    planes = mesh.shape["pts"] // PLANE
    placed = tuple(P(SITE_PTS, *[None] * n) for n in (4, 1, 0, 2, 2, 1, 2))
    return jax.shard_map(
        functools.partial(local, planes),
        mesh=mesh,
        in_specs=placed,
        out_specs=P(SITE_PTS, None, None, None),
        check_vma=False,
    )
```

```python
import functools

import jax
import jax.numpy as jnp
import numpy as np
from jax import lax
from jax.experimental import pallas as pl
from jax.experimental.pallas import tpu as pltpu
from jax.sharding import PartitionSpec as P

MESH = pl.DeviceIdType.MESH
HIGHEST = lax.Precision.HIGHEST
SITE_PTS = ("site", "pts")
PLANE = 8
LIMIT = 6.0
TOP = 32767.0
CHUNK = 4
BLOCKS = 16
VMEM_LIMIT = 60 * 1024 * 1024


def mate(j, e):
    for bit in (1, 2, 4):
        if e & bit:
            j = j + bit * (1 - 2 * ((j // bit) % 2))
    return j


def partner(index):
    return {"pts": index}


def train_of(planes):
    half = planes // 2
    dz = np.arange(planes * PLANE) // PLANE
    e = np.arange(planes * PLANE) % PLANE
    up = ((dz >= 1) & (dz < half)) | ((dz == half) & (e < PLANE // 2))
    down = (dz > half) | ((dz == half) & (e >= PLANE // 2))
    distance = np.where(up, dz, np.where(down, planes - dz, 0))
    return distance, up.astype(np.int32) - down.astype(np.int32), e


def before_table(planes):
    distance, way, e = train_of(planes)
    same = (way[:, None] == way[None, :]) & (way[:, None] != 0)
    ahead = (distance[:, None] > distance[None, :]) | (
        (distance[:, None] == distance[None, :]) & (e[:, None] < e[None, :])
    )
    return (same & ahead).astype(np.float32)


def reach_tables(planes, caps):
    distance, way, e = train_of(planes)
    half = planes // 2
    size = planes * PLANE
    reach = np.zeros((size, size), np.float32)
    limit = np.full((4 * planes, size), 1e6, np.float32)
    for chip in range(4):
        turned = np.arange(size) ^ (2 * chip)
        for s in range(1, half + 1):
            for w, sign in enumerate((1, -1)):
                column = chip * planes + w * half + s - 1
                reach[:, column] = ((way == sign) & (distance >= s))[turned]
                limit[chip * planes : (chip + 1) * planes, column] = caps[s - 1]
    return reach, limit


def most_packets(planes):
    half = planes // 2
    return tuple(2 * (PLANE * (half - s) + PLANE // 2) for s in range(1, half + 1))


def turn_blocks(value):
    rows, size = value.shape
    skewed = pltpu.roll(value, 0, 1, stride=8, stride_axis=0)
    row = lax.broadcasted_iota(jnp.int32, value.shape, 0)
    block = lax.broadcasted_iota(jnp.int32, value.shape, 1) // 8
    turned = jnp.zeros_like(value)
    for n in range(rows):
        picked = jnp.where(block == ((row + n) & (rows - 1)), skewed, 0.0)
        picked = jnp.sum(picked, axis=0, keepdims=True)
        if n:
            picked = pltpu.roll(picked, size - 8 * n, 1)
        turned = jnp.where(row == n, picked, turned)
    return turned


def exchange_kernel(
    planes, list_ref, count_ref, moment_ref, onset_ref, slip_ref, before_ref, reach_ref, limit_ref, green_ref,
    tab_ref, block_ref, place_ref, over_ref, start_ref, rest_ref, weight_ref, other_ref,
    row_ref, rows_ref, send_a, recv_a, send_b, recv_b, send_g, recv_g,
):
    me = lax.axis_index("pts")
    z, j = me // PLANE, me % PLANE
    size = planes * PLANE
    listed = list_ref.shape[1]
    strains = moment_ref.shape[1]

    barrier = pltpu.get_barrier_semaphore()
    for e in range(1, PLANE):
        pl.semaphore_signal(
            barrier, inc=1, device_id=partner(z * PLANE + mate(j, e)), device_id_type=MESH
        )
    for d in range(1, planes):
        pl.semaphore_signal(
            barrier, inc=1, device_id=partner(((z + d) % planes) * PLANE + j), device_id_type=MESH
        )
    entry = lax.broadcasted_iota(jnp.int32, (1, listed), 1)
    names = jnp.where(entry < count_ref[0], list_ref[...], -1).astype(jnp.float32)
    row_ref[...] = jnp.zeros_like(row_ref)
    row_ref[0, :, pl.ds(0, listed)] = names
    row_ref[0, :, pl.ds(listed + 1, strains)] = moment_ref[...]
    rows_ref[pl.ds(0, 1)] = row_ref[...]
    pl.semaphore_wait(barrier, PLANE - 1 + planes - 1)

    copies = []
    for e in range(1, PLANE):
        copies.append(
            pltpu.make_async_remote_copy(
                src_ref=row_ref,
                dst_ref=rows_ref.at[pl.ds(e, 1)],
                send_sem=send_a.at[e],
                recv_sem=recv_a.at[e],
                device_id=partner(z * PLANE + mate(j, e)),
                device_id_type=MESH,
            )
        )
    for copy in copies:
        copy.start()
    green = pltpu.make_async_remote_copy(
        src_ref=green_ref,
        dst_ref=other_ref,
        send_sem=send_g,
        recv_sem=recv_g,
        device_id=partner(z * PLANE + mate(j, 1)),
        device_id_type=MESH,
    )
    green.start()
    for copy in copies:
        copy.wait()
    copies = []
    for d in range(1, planes):
        copies.append(
            pltpu.make_async_remote_copy(
                src_ref=rows_ref.at[pl.ds(0, PLANE)],
                dst_ref=rows_ref.at[pl.ds((planes - d) * PLANE, PLANE)],
                send_sem=send_b.at[d],
                recv_sem=recv_b.at[d],
                device_id=partner(((z + d) % planes) * PLANE + j),
                device_id_type=MESH,
            )
        )
    for copy in copies:
        copy.start()
    onset = turn_blocks(onset_ref[...].astype(jnp.float32)).astype(jnp.int32)
    start_ref[...] = 8 - 2 * (onset >> 7)
    rest_ref[...] = onset & 127
    weight_ref[...] = turn_blocks(slip_ref[...])
    for copy in copies:
        copy.wait()

    turned = rows_ref[...].reshape(size, 128).T
    named = turned[:listed]
    holder = jnp.floor(named * (1.0 / BLOCKS))
    source = lax.broadcasted_iota(jnp.int32, (size, size), 0)
    lane = lax.broadcasted_iota(jnp.int32, (size, size), 1)
    at = (z + planes - (source & (planes - 1))) & (planes - 1)
    source_id = (at * PLANE + (j ^ (source // planes))).astype(jnp.float32)
    active = jnp.zeros((size, size), jnp.float32)
    for k in range(listed):
        active = active + jnp.where(holder[k : k + 1, :] == source_id, 1.0, 0.0)
    view = pltpu.roll(active, 0, 1, stride=PLANE, stride_axis=0)
    chips = jnp.concatenate(
        [
            view[2 * g * planes : (2 * g + 1) * planes] + view[(2 * g + 1) * planes : (2 * g + 2) * planes]
            for g in range(4)
        ],
        axis=0,
    ).astype(jnp.bfloat16)
    counts = jnp.dot(chips, reach_ref[...], preferred_element_type=jnp.float32)
    excess = jnp.max(counts - limit_ref[...], axis=0, keepdims=True)
    excess = jnp.max(excess, axis=1, keepdims=True)
    over_ref[...] = jnp.where(excess > 0.5, 1, 0).astype(jnp.int32)

    first = jnp.dot(chips[:planes], before_ref[...], preferred_element_type=jnp.float32)
    second = first + view[:planes]
    diagonal = (lane[:planes] // PLANE) == source[:planes]
    part = lax.broadcasted_iota(jnp.int32, (8, size), 0)
    place = jnp.where(
        part == 0,
        jnp.sum(jnp.where(diagonal, first, 0.0), axis=0, keepdims=True),
        jnp.sum(jnp.where(diagonal, second, 0.0), axis=0, keepdims=True),
    )
    place_ref[...] = place.astype(jnp.int32)

    moment = turned[32:40]
    bound = LIMIT * jnp.sum(
        jnp.where((part >= 1) & (part <= strains), jnp.abs(moment), 0.0), axis=0, keepdims=True
    )
    gain = 1.0 / jnp.maximum(bound, 1e-30)
    moment = jnp.where(part == 7, gain, moment)
    side = lane[:1]
    way = jnp.where(side < PLANE, 0, jnp.where(side < (planes // 2) * PLANE + PLANE // 2, 1, -1))
    mine = way == 1 - 2 * (j % 2)
    slot = source.astype(jnp.float32)

    def info(owner, shift):
        owner = owner.astype(jnp.float32)
        block = jnp.where(holder == owner, named - (BLOCKS * owner - shift), 0.0)
        return jnp.where(part == 0, jnp.sum(block, axis=0, keepdims=True), moment)

    def table(which, held, position):
        chosen = (held > 0.5) & mine & (position == slot)
        return lax.dot_general(
            which,
            jnp.where(chosen, 1.0, 0.0),
            (((1,), (1,)), ((), ())),
            precision=HIGHEST,
            preferred_element_type=jnp.float32,
        )

    own = info(me, 0.0)
    both = table(own, view[:1], first[:1]) + table(
        info(me + 1 - 2 * (j % 2), float(BLOCKS)), view[planes : planes + 1], second[:1]
    )
    tab_ref[:, :size] = both
    tab_ref[:, size:] = own
    block_ref[:, :size] = both.astype(jnp.int32)
    block_ref[:, size:] = own.astype(jnp.int32)
    green.wait()


def exchange(planes, caps, lists, count, moment, onset, slip, green):
    size = planes * PLANE
    before = before_table(planes)
    reach, limit = reach_tables(planes, caps)
    vmem = pl.BlockSpec(memory_space=pltpu.VMEM)
    smem = pl.BlockSpec(memory_space=pltpu.SMEM)
    hbm = pl.BlockSpec(memory_space=pl.ANY)
    return pl.pallas_call(
        functools.partial(exchange_kernel, planes),
        out_shape=(
            jax.ShapeDtypeStruct((8, 2 * size), jnp.float32),
            jax.ShapeDtypeStruct((8, 2 * size), jnp.int32),
            jax.ShapeDtypeStruct((8, size), jnp.int32),
            jax.ShapeDtypeStruct((1, 1), jnp.int32),
            jax.ShapeDtypeStruct(onset.shape, jnp.int32),
            jax.ShapeDtypeStruct(onset.shape, jnp.int32),
            jax.ShapeDtypeStruct(slip.shape, jnp.float32),
            jax.ShapeDtypeStruct(green.shape, green.dtype),
        ),
        in_specs=[vmem, smem, vmem, vmem, vmem, vmem, vmem, vmem, hbm],
        out_specs=(vmem, vmem, vmem, vmem, vmem, vmem, vmem, hbm),
        scratch_shapes=[
            pltpu.VMEM((1, 1, 128), jnp.float32),
            pltpu.VMEM((size, 1, 128), jnp.float32),
            pltpu.SemaphoreType.DMA((PLANE,)),
            pltpu.SemaphoreType.DMA((PLANE,)),
            pltpu.SemaphoreType.DMA((planes,)),
            pltpu.SemaphoreType.DMA((planes,)),
            pltpu.SemaphoreType.DMA,
            pltpu.SemaphoreType.DMA,
        ],
        compiler_params=pltpu.CompilerParams(collective_id=0, has_side_effects=True),
        name="exchange",
    )(
        lists, count, moment, onset, slip, jnp.asarray(before, jnp.bfloat16), jnp.asarray(reach, jnp.bfloat16),
        jnp.asarray(limit), green,
    )


RELAYED = 6


def spans(count):
    return [(first, min(first + CHUNK, count)) for first in range(0, count, CHUNK)]


def carry_kernel(planes, caps, place_ref, block_ref, tab_ref, mine_ref, other_ref, out_ref, *scratch):
    half = planes // 2
    green, own, staged, near, relay = scratch[:5]
    moved = scratch[5 : 5 + half]
    (load, send_z, recv_z, send_x, recv_x, send_n, recv_n, send_r, recv_r, send_f) = scratch[5 + half :]
    me = lax.axis_index("pts")
    z, j = me // PLANE, me % PLANE
    w = j % 2
    size = planes * PLANE

    loads = [
        pltpu.make_async_copy(mine_ref, green.at[pl.ds(0, BLOCKS)], load.at[0]),
        pltpu.make_async_copy(other_ref, green.at[pl.ds(BLOCKS, BLOCKS)], load.at[1]),
    ]
    for copy in loads:
        copy.start()
    barrier = pltpu.get_barrier_semaphore()
    for e in range(1, PLANE):
        pl.semaphore_signal(
            barrier, inc=1, device_id=partner(z * PLANE + mate(j, e)), device_id_type=MESH
        )
    for way in (1, planes - 1):
        pl.semaphore_signal(
            barrier, inc=1, device_id=partner(((z + way) % planes) * PLANE + j), device_id_type=MESH
        )
    for copy in loads:
        copy.wait()
    pl.semaphore_wait(barrier, PLANE - 1 + 2)

    def trace(entry, write):
        block = jnp.clip(block_ref[0, entry], 0, 2 * BLOCKS - 1)
        moment = [tab_ref[1 + s, entry] for s in range(6)]
        gain = tab_ref[7, entry]
        for p in range(4):
            total = moment[0] * green[block, p, 0].astype(jnp.float32)
            for s in range(1, 6):
                total = total + moment[s] * green[block, p, s].astype(jnp.float32)
            root = lax.rsqrt(lax.rsqrt(jnp.abs(total) * gain))
            level = jnp.minimum(root * TOP, TOP)
            code = jnp.round(jnp.where(total < 0.0, -level, level)).astype(jnp.int32)
            write(p, code.astype(jnp.int16))

    def hop(s, c):
        first, last = spans(caps[s])[c]
        source = own if s == 0 else moved[s - 1]
        return pltpu.make_async_remote_copy(
            src_ref=source.at[pl.ds(first, last - first)],
            dst_ref=moved[s].at[pl.ds(first, last - first)],
            send_sem=send_z.at[s, c],
            recv_sem=recv_z.at[s, c],
            device_id=partner(((z + 1 + w * (planes - 2)) % planes) * PLANE + j),
            device_id_type=MESH,
        )

    def offset(s):
        return (s + 1) + w * (planes - 2 * (s + 1))

    def spread(s, e):
        return pltpu.make_async_remote_copy(
            src_ref=staged.at[s, e],
            dst_ref=out_ref.at[offset(s), pl.ds(e - e % 2, 2)],
            send_sem=send_x.at[s, e],
            recv_sem=recv_x.at[offset(s), e // 2],
            device_id=partner(z * PLANE + mate(j, e)),
            device_id_type=MESH,
        )

    beside = (j // 2 + 1 + 2 * w) % 4

    def hand(s):
        return pltpu.make_async_remote_copy(
            src_ref=staged.at[s, pl.ds(4, 2)],
            dst_ref=relay.at[s],
            send_sem=send_r.at[s],
            recv_sem=recv_r.at[s],
            device_id=partner(z * PLANE + beside * 2 + w),
            device_id_type=MESH,
        )

    def onward(s, i):
        return pltpu.make_async_remote_copy(
            src_ref=relay.at[s, i],
            dst_ref=out_ref.at[offset(s), pl.ds(4, 2)],
            send_sem=send_f.at[s, i],
            recv_sem=recv_x.at[offset(s), 2],
            device_id=partner(z * PLANE + beside * 2 + w + i * (1 - 2 * w)),
            device_id_type=MESH,
        )

    def pass_on(s):
        hand(s).wait_recv()
        for i in range(2):
            onward(s, i).start()

    def visit(e):
        return pltpu.make_async_remote_copy(
            src_ref=near.at[e],
            dst_ref=out_ref.at[0, e],
            send_sem=send_n.at[e],
            recv_sem=recv_n.at[e],
            device_id=partner(z * PLANE + mate(j, e)),
            device_id_type=MESH,
        )

    for c, (first, last) in enumerate(spans(caps[0])):

        def fill(i, carry):
            def write(p, code):
                own[i, pl.ds(16 * p, 16), :] = code

            trace(i, write)
            return carry

        lax.fori_loop(first, last, fill, 0)
        hop(0, c).start()

    def write_own(p, code):
        out_ref[0, 0, pl.ds(16 * p, 16), :] = code

    trace(size, write_own)

    def fill_near(e, carry):
        def write(p, code):
            near[e, pl.ds(16 * p, 16), :] = code

        trace(size + e, write)
        return carry

    lax.fori_loop(1, PLANE, fill_near, 0)
    for e in range(1, PLANE):
        visit(e).start()

    def deliver(s, mates):
        q = offset(s)
        for e in mates:
            for r in range(2):
                at = jnp.clip(place_ref[r, q * PLANE + e], 0, caps[s] - 1)
                packet = moved[s][at]
                if e == 0:
                    out_ref[q, r] = packet
                else:
                    staged[s, e, (e + r) % 2] = packet
        if s < RELAYED:
            hand(s).start()
        for e in mates:
            if e and not (s < RELAYED and e // 2 == 2):
                spread(s, e).start()

    low, high = range(PLANE // 2), range(PLANE // 2, PLANE)
    for s in range(half):
        for c, (first, last) in enumerate(spans(caps[s])):
            hop(s, c).wait_recv()
            if s + 1 < half and first < caps[s + 1]:
                hop(s + 1, c).start()
        if s + 1 < half:
            deliver(s, range(PLANE))
            if 0 < s <= RELAYED:
                pass_on(s - 1)
        else:

            @pl.when(w == 0)
            def _():
                deliver(half - 1, low)

            @pl.when(w == 1)
            def _():
                deliver(half - 1, high)

    for s in range(half):
        for c in range(len(spans(caps[s]))):
            hop(s, c).wait_send()
    for e in range(1, PLANE):
        visit(e).wait()
        for s in range(half - 1):
            if not (s < RELAYED and e // 2 == 2):
                spread(s, e).wait_send()
    for s in range(RELAYED):
        hand(s).wait_send()
        for i in range(2):
            onward(s, i).wait_send()

    @pl.when(w == 0)
    def _():
        for e in low:
            if e:
                spread(half - 1, e).wait_send()

    @pl.when(w == 1)
    def _():
        for e in high:
            spread(half - 1, e).wait_send()

    def arrival(q, chip):
        return pltpu.make_async_remote_copy(
            src_ref=staged.at[0, 1],
            dst_ref=out_ref.at[q, pl.ds(2 * chip, 2)],
            send_sem=send_x.at[0, 1],
            recv_sem=recv_x.at[q, chip],
            device_id=partner(z * PLANE + mate(j, 1)),
            device_id_type=MESH,
        )

    for q in range(1, planes):
        for chip in range(1, 4):
            arrival(q, chip).wait_recv()

    @pl.when(w == 1)
    def _():
        for q in range(1, half + 1):
            arrival(q, 0).wait_recv()

    @pl.when(w == 0)
    def _():
        for q in range(half + 1, planes):
            arrival(q, 0).wait_recv()


def carry(planes, caps, number, place, block, tab, mine, other):
    half = planes // 2
    chunks = len(spans(caps[0]))
    smem = pl.BlockSpec(memory_space=pltpu.SMEM)
    hbm = pl.BlockSpec(memory_space=pl.ANY)
    packet = (64, 128)
    return pl.pallas_call(
        functools.partial(carry_kernel, planes, caps),
        out_shape=jax.ShapeDtypeStruct((planes, PLANE, *packet), jnp.int16),
        in_specs=[smem, smem, smem, hbm, hbm],
        out_specs=pl.BlockSpec(memory_space=pltpu.VMEM),
        scratch_shapes=[
            pltpu.VMEM((2 * mine.shape[0], *mine.shape[1:]), mine.dtype),
            pltpu.VMEM((caps[0], *packet), jnp.int16),
            pltpu.VMEM((half, PLANE, 2, *packet), jnp.int16),
            pltpu.VMEM((PLANE, *packet), jnp.int16),
            pltpu.VMEM((RELAYED, 2, 2, *packet), jnp.int16),
            *[pltpu.VMEM((caps[s], *packet), jnp.int16) for s in range(half)],
            pltpu.SemaphoreType.DMA((2,)),
            pltpu.SemaphoreType.DMA((half, chunks)),
            pltpu.SemaphoreType.DMA((half, chunks)),
            pltpu.SemaphoreType.DMA((half, PLANE)),
            pltpu.SemaphoreType.DMA((planes, 4)),
            pltpu.SemaphoreType.DMA((PLANE,)),
            pltpu.SemaphoreType.DMA((PLANE,)),
            pltpu.SemaphoreType.DMA((RELAYED,)),
            pltpu.SemaphoreType.DMA((RELAYED,)),
            pltpu.SemaphoreType.DMA((RELAYED, 2)),
        ],
        compiler_params=pltpu.CompilerParams(
            collective_id=number, has_side_effects=True, vmem_limit_bytes=VMEM_LIMIT
        ),
        name="carry",
    )(place, block, tab, mine, other)


def halves(value):
    coarse = value.astype(jnp.bfloat16)
    return coarse, (value - coarse.astype(jnp.float32)).astype(jnp.bfloat16)


def motion_kernel(
    planes, list_ref, count_ref, start_ref, rest_ref, slip_ref, moment_ref, packet_ref, rate_ref, out_ref,
    near, far, motion,
):
    me = lax.axis_index("pts")
    z, j = me // PLANE, me % PLANE
    variations = out_ref.shape[0]
    bound = jnp.abs(moment_ref[0, 0])
    for s in range(1, 6):
        bound = bound + jnp.abs(moment_ref[0, s])
    lane = lax.broadcasted_iota(jnp.int32, (16, 128), 1)
    motion[...] = jnp.zeros_like(motion)
    near[...] = jnp.zeros_like(near)
    far[...] = jnp.zeros_like(far)
    count = count_ref[0]

    def add_blocks(pair, carry):
        for n in range(2):
            k = 2 * pair + n
            holder = list_ref[0, k] // BLOCKS
            q = (z - holder // PLANE + planes) % planes
            e = j ^ (holder % PLANE)
            unit = jnp.where(k < count, bound, 0.0) * (LIMIT / TOP**4)
            for p in range(4):
                code = packet_ref[q, e, pl.ds(16 * p, 16), :].astype(jnp.int32).astype(jnp.float32)
                square = code * jnp.abs(code)
                trace = square * jnp.abs(square) * unit
                near[4 * n + p, pl.ds(8, 16), :] = trace
                far[4 * n + p, pl.ds(10, 16), :] = trace
        for v in range(variations):
            total = None
            for i in range(8):
                start = start_ref[pair, v * 8 + i]
                rest = rest_ref[pair, v * 8 + i]
                trace = jnp.where(
                    lane + rest < 128, near[i, pl.ds(start, 16), :], far[i, pl.ds(start, 16), :]
                )
                term = slip_ref[pair, v * 8 + i] * pltpu.roll(trace, rest, 1)
                total = term if total is None else total + term
            motion[v, pl.ds(8, 16), :] += total
        return carry

    lax.fori_loop(0, (count + 1) // 2, add_blocks, 0)

    row = lax.broadcasted_iota(jnp.int32, (128, 128), 0)
    column = lax.broadcasted_iota(jnp.int32, (128, 128), 1)
    for v in range(variations):
        rate = jnp.broadcast_to(rate_ref[pl.ds(v, 1), :], (128, 128))
        rate = pltpu.roll(rate, 0, 1, stride=1, stride_axis=0)
        taps = jnp.concatenate(
            [jnp.where(column >= row, rate, 0.0), jnp.where(column < row, rate, 0.0)], axis=0
        )
        signal = jnp.concatenate([motion[v, pl.ds(8, 16), :], motion[v, pl.ds(6, 16), :]], axis=1)
        coarse, fine = halves(signal)
        taps, rest = halves(taps)
        both = jnp.dot(
            jnp.concatenate([coarse, fine], axis=0), taps, preferred_element_type=jnp.float32
        )
        out_ref[v] = (
            both[:16] + both[16:] + jnp.dot(coarse, rest, preferred_element_type=jnp.float32)
        )


def synthesize(planes, block_list, count, start, rest, slip, moment, packets, rate):
    variations = slip.shape[0]
    smem = pl.BlockSpec(memory_space=pltpu.SMEM)
    vmem = pl.BlockSpec(memory_space=pltpu.VMEM)
    return pl.pallas_call(
        functools.partial(motion_kernel, planes),
        out_shape=jax.ShapeDtypeStruct((variations, 16, 128), jnp.float32),
        in_specs=[smem, smem, smem, smem, smem, smem, vmem, vmem],
        out_specs=vmem,
        scratch_shapes=[
            pltpu.VMEM((8, 24, 128), jnp.float32),
            pltpu.VMEM((8, 32, 128), jnp.float32),
            pltpu.VMEM((variations, 24, 128), jnp.float32),
        ],
        compiler_params=pltpu.CompilerParams(vmem_limit_bytes=VMEM_LIMIT),
        name="synthesize",
    )(block_list, count, start, rest, slip, moment, packets, rate)


CAPS = (36, 33, 29, 26, 22, 18, 13, 8)


def local(planes, green_tensors, block_lists, block_count, onset_steps, slip_amount, mechanism, slip_rate):
    held, points, strains, parts, length = green_tensors.shape
    green = green_tensors.reshape(held, points, strains, parts, length // 128, 128)
    green = green.transpose(0, 1, 2, 4, 3, 5).reshape(held, points, strains, -1, 128)
    tab, block, place, over, start, rest, weight, other = exchange(
        planes, CAPS, block_lists, block_count, mechanism, onset_steps[0], slip_amount[0], green
    )
    packets = lax.cond(
        over[0, 0] > 0,
        functools.partial(carry, planes, most_packets(planes), 1),
        functools.partial(carry, planes, CAPS, 2),
        place,
        block,
        tab,
        green,
        other,
    )
    seis = synthesize(
        planes, block_lists, block_count, start, rest, weight, mechanism, packets, slip_rate[0]
    )
    seis = seis.reshape(-1, length // 128, parts, 128).transpose(0, 2, 1, 3)
    return seis.reshape(1, -1, parts, length)


def solution(mesh):
    planes = mesh.shape["pts"] // PLANE
    placed = tuple(P(SITE_PTS, *[None] * n) for n in (4, 1, 0, 2, 2, 1, 2))
    return jax.shard_map(
        functools.partial(local, planes),
        mesh=mesh,
        in_specs=placed,
        out_specs=P(SITE_PTS, None, None, None),
        check_vma=False,
    )
```

```python
import functools

import jax
import jax.numpy as jnp
import numpy as np
from jax import lax
from jax.experimental import pallas as pl
from jax.experimental.pallas import tpu as pltpu
from jax.sharding import PartitionSpec as P

MESH = pl.DeviceIdType.MESH
HIGHEST = lax.Precision.HIGHEST
SITE_PTS = ("site", "pts")
PLANE = 8
LIMIT = 6.0
TOP = 32767.0
CHUNK = 4
BLOCKS = 16
VMEM_LIMIT = 60 * 1024 * 1024


def mate(j, e):
    for bit in (1, 2, 4):
        if e & bit:
            j = j + bit * (1 - 2 * ((j // bit) % 2))
    return j


def partner(index):
    return {"pts": index}


def train_of(planes):
    half = planes // 2
    dz = np.arange(planes * PLANE) // PLANE
    e = np.arange(planes * PLANE) % PLANE
    up = ((dz >= 1) & (dz < half)) | ((dz == half) & (e < PLANE // 2))
    down = (dz > half) | ((dz == half) & (e >= PLANE // 2))
    distance = np.where(up, dz, np.where(down, planes - dz, 0))
    return distance, up.astype(np.int32) - down.astype(np.int32), e


def before_table(planes):
    distance, way, e = train_of(planes)
    same = (way[:, None] == way[None, :]) & (way[:, None] != 0)
    ahead = (distance[:, None] > distance[None, :]) | (
        (distance[:, None] == distance[None, :]) & (e[:, None] < e[None, :])
    )
    return (same & ahead).astype(np.float32)


def reach_tables(planes, caps):
    distance, way, e = train_of(planes)
    half = planes // 2
    size = planes * PLANE
    reach = np.zeros((size, size), np.float32)
    limit = np.full((4 * planes, size), 1e6, np.float32)
    for chip in range(4):
        turned = np.arange(size) ^ (2 * chip)
        for s in range(1, half + 1):
            for w, sign in enumerate((1, -1)):
                column = chip * planes + w * half + s - 1
                reach[:, column] = ((way == sign) & (distance >= s))[turned]
                limit[chip * planes : (chip + 1) * planes, column] = caps[s - 1]
    return reach, limit


def most_packets(planes):
    half = planes // 2
    return tuple(2 * (PLANE * (half - s) + PLANE // 2) for s in range(1, half + 1))


def turn_blocks(value):
    rows, size = value.shape
    skewed = pltpu.roll(value, 0, 1, stride=8, stride_axis=0)
    row = lax.broadcasted_iota(jnp.int32, value.shape, 0)
    block = lax.broadcasted_iota(jnp.int32, value.shape, 1) // 8
    turned = jnp.zeros_like(value)
    for n in range(rows):
        picked = jnp.where(block == ((row + n) & (rows - 1)), skewed, 0.0)
        picked = jnp.sum(picked, axis=0, keepdims=True)
        if n:
            picked = pltpu.roll(picked, size - 8 * n, 1)
        turned = jnp.where(row == n, picked, turned)
    return turned


def spans(count):
    return [(first, min(first + CHUNK, count)) for first in range(0, count, CHUNK)]


def carry_kernel(
    planes, caps, list_ref, count_ref, moment_ref, onset_ref, slip_ref, before_ref, reach_ref,
    limit_ref, green_ref, out_ref, over_ref, start_ref, rest_ref, weight_ref, *scratch,
):
    half = planes // 2
    (row_ref, rows_ref, tab_made, block_made, place_made, tab_ref, block_ref, place_ref) = scratch[:8]
    green, own, staged, near = scratch[8:12]
    moved = scratch[12 : 12 + half]
    (
        send_a, recv_a, send_b, recv_b, send_g, recv_g, load_sem, table_sem,
        send_z, recv_z, send_x, recv_x, send_n, recv_n,
    ) = scratch[12 + half :]
    me = lax.axis_index("pts")
    z, j = me // PLANE, me % PLANE
    size = planes * PLANE
    listed = list_ref.shape[1]
    strains = moment_ref.shape[1]

    load = pltpu.make_async_copy(green_ref, green.at[pl.ds(0, BLOCKS)], load_sem)
    load.start()
    barrier = pltpu.get_barrier_semaphore()
    for e in range(1, PLANE):
        pl.semaphore_signal(
            barrier, inc=1, device_id=partner(z * PLANE + mate(j, e)), device_id_type=MESH
        )
    for d in range(1, planes):
        pl.semaphore_signal(
            barrier, inc=1, device_id=partner(((z + d) % planes) * PLANE + j), device_id_type=MESH
        )
    entry = lax.broadcasted_iota(jnp.int32, (1, listed), 1)
    names = jnp.where(entry < count_ref[0], list_ref[...], -1).astype(jnp.float32)
    row_ref[...] = jnp.zeros_like(row_ref)
    row_ref[0, :, pl.ds(0, listed)] = names
    row_ref[0, :, pl.ds(listed + 1, strains)] = moment_ref[...]
    rows_ref[pl.ds(0, 1)] = row_ref[...]
    pl.semaphore_wait(barrier, PLANE - 1 + planes - 1)

    copies = []
    for e in range(1, PLANE):
        copies.append(
            pltpu.make_async_remote_copy(
                src_ref=row_ref,
                dst_ref=rows_ref.at[pl.ds(e, 1)],
                send_sem=send_a.at[e],
                recv_sem=recv_a.at[e],
                device_id=partner(z * PLANE + mate(j, e)),
                device_id_type=MESH,
            )
        )
    for copy in copies:
        copy.start()
    other = pltpu.make_async_remote_copy(
        src_ref=green_ref,
        dst_ref=green.at[pl.ds(BLOCKS, BLOCKS)],
        send_sem=send_g,
        recv_sem=recv_g,
        device_id=partner(z * PLANE + mate(j, 1)),
        device_id_type=MESH,
    )
    other.start()
    for copy in copies:
        copy.wait()
    copies = []
    for d in range(1, planes):
        copies.append(
            pltpu.make_async_remote_copy(
                src_ref=rows_ref.at[pl.ds(0, PLANE)],
                dst_ref=rows_ref.at[pl.ds((planes - d) * PLANE, PLANE)],
                send_sem=send_b.at[d],
                recv_sem=recv_b.at[d],
                device_id=partner(((z + d) % planes) * PLANE + j),
                device_id_type=MESH,
            )
        )
    for copy in copies:
        copy.start()
    onset = turn_blocks(onset_ref[...].astype(jnp.float32)).astype(jnp.int32)
    start_ref[...] = 8 - 2 * (onset >> 7)
    rest_ref[...] = onset & 127
    weight_ref[...] = turn_blocks(slip_ref[...])
    for copy in copies:
        copy.wait()

    turned = rows_ref[...].reshape(size, 128).T
    named = turned[:listed]
    holder = jnp.floor(named * (1.0 / BLOCKS))
    source = lax.broadcasted_iota(jnp.int32, (size, size), 0)
    lane = lax.broadcasted_iota(jnp.int32, (size, size), 1)
    at = (z + planes - (source & (planes - 1))) & (planes - 1)
    source_id = (at * PLANE + (j ^ (source // planes))).astype(jnp.float32)
    active = jnp.zeros((size, size), jnp.float32)
    for k in range(listed):
        active = active + jnp.where(holder[k : k + 1, :] == source_id, 1.0, 0.0)
    view = pltpu.roll(active, 0, 1, stride=PLANE, stride_axis=0)
    chips = jnp.concatenate(
        [
            view[2 * g * planes : (2 * g + 1) * planes] + view[(2 * g + 1) * planes : (2 * g + 2) * planes]
            for g in range(4)
        ],
        axis=0,
    ).astype(jnp.bfloat16)
    counts = jnp.dot(chips, reach_ref[...], preferred_element_type=jnp.float32)
    excess = jnp.max(counts - limit_ref[...], axis=0, keepdims=True)
    excess = jnp.max(excess, axis=1, keepdims=True)
    over_ref[...] = jnp.where(excess > 0.5, 1, 0).astype(jnp.int32)

    first = jnp.dot(chips[:planes], before_ref[...], preferred_element_type=jnp.float32)
    second = first + view[:planes]
    diagonal = (lane[:planes] // PLANE) == source[:planes]
    part = lax.broadcasted_iota(jnp.int32, (8, size), 0)
    place = jnp.where(
        part == 0,
        jnp.sum(jnp.where(diagonal, first, 0.0), axis=0, keepdims=True),
        jnp.sum(jnp.where(diagonal, second, 0.0), axis=0, keepdims=True),
    )
    place_made[...] = place.astype(jnp.int32)

    moment = turned[32:40]
    bound = LIMIT * jnp.sum(
        jnp.where((part >= 1) & (part <= strains), jnp.abs(moment), 0.0), axis=0, keepdims=True
    )
    gain = 1.0 / jnp.maximum(bound, 1e-30)
    moment = jnp.where(part == 7, gain, moment)
    side = lane[:1]
    way = jnp.where(side < PLANE, 0, jnp.where(side < (planes // 2) * PLANE + PLANE // 2, 1, -1))
    mine = way == 1 - 2 * (j % 2)
    slot = source.astype(jnp.float32)

    def info(owner, shift):
        owner = owner.astype(jnp.float32)
        block = jnp.where(holder == owner, named - (BLOCKS * owner - shift), 0.0)
        return jnp.where(part == 0, jnp.sum(block, axis=0, keepdims=True), moment)

    def table(which, held, position):
        chosen = (held > 0.5) & mine & (position == slot)
        return lax.dot_general(
            which,
            jnp.where(chosen, 1.0, 0.0),
            (((1,), (1,)), ((), ())),
            precision=HIGHEST,
            preferred_element_type=jnp.float32,
        )

    own_info = info(me, 0.0)
    both = table(own_info, view[:1], first[:1]) + table(
        info(me + 1 - 2 * (j % 2), float(BLOCKS)), view[planes : planes + 1], second[:1]
    )
    tab_made[:, :size] = both
    tab_made[:, size:] = own_info
    block_made[:, :size] = both[:1].astype(jnp.int32)
    block_made[:, size:] = own_info[:1].astype(jnp.int32)
    tables = [
        pltpu.make_async_copy(made, held, table_sem.at[n])
        for n, (made, held) in enumerate(
            ((tab_made, tab_ref), (block_made, block_ref), (place_made, place_ref))
        )
    ]
    for copy in tables:
        copy.start()
    other.wait()
    load.wait()
    for copy in tables:
        copy.wait()

    w = j % 2

    def trace(entry, write):
        block = jnp.clip(block_ref[0, entry], 0, 2 * BLOCKS - 1)
        moment = [tab_ref[1 + s, entry] for s in range(6)]
        gain = tab_ref[7, entry]
        for p in range(4):
            total = moment[0] * green[block, p, 0].astype(jnp.float32)
            for s in range(1, 6):
                total = total + moment[s] * green[block, p, s].astype(jnp.float32)
            root = lax.rsqrt(lax.rsqrt(jnp.abs(total) * gain))
            level = jnp.minimum(root * TOP, TOP)
            code = jnp.round(jnp.where(total < 0.0, -level, level)).astype(jnp.int32)
            write(p, code.astype(jnp.int16))

    def hop(s, c):
        first, last = spans(caps[s])[c]
        source = own if s == 0 else moved[s - 1]
        return pltpu.make_async_remote_copy(
            src_ref=source.at[pl.ds(first, last - first)],
            dst_ref=moved[s].at[pl.ds(first, last - first)],
            send_sem=send_z.at[s, c],
            recv_sem=recv_z.at[s, c],
            device_id=partner(((z + 1 + w * (planes - 2)) % planes) * PLANE + j),
            device_id_type=MESH,
        )

    def offset(s):
        return (s + 1) + w * (planes - 2 * (s + 1))

    def spread(s, e):
        return pltpu.make_async_remote_copy(
            src_ref=staged.at[s, e],
            dst_ref=out_ref.at[offset(s), pl.ds(e - e % 2, 2)],
            send_sem=send_x.at[s, e],
            recv_sem=recv_x.at[offset(s), e // 2],
            device_id=partner(z * PLANE + mate(j, e)),
            device_id_type=MESH,
        )

    def visit(e):
        return pltpu.make_async_remote_copy(
            src_ref=near.at[e],
            dst_ref=out_ref.at[0, e],
            send_sem=send_n.at[e],
            recv_sem=recv_n.at[e],
            device_id=partner(z * PLANE + mate(j, e)),
            device_id_type=MESH,
        )

    for c, (first, last) in enumerate(spans(caps[0])):

        def fill(i, carry):
            def write(p, code):
                own[i, pl.ds(16 * p, 16), :] = code

            trace(i, write)
            return carry

        lax.fori_loop(first, last, fill, 0)
        hop(0, c).start()

    def write_own(p, code):
        out_ref[0, 0, pl.ds(16 * p, 16), :] = code

    trace(size, write_own)

    def fill_near(e, carry):
        def write(p, code):
            near[e, pl.ds(16 * p, 16), :] = code

        trace(size + e, write)
        return carry

    lax.fori_loop(1, PLANE, fill_near, 0)
    for e in range(1, PLANE):
        visit(e).start()

    def deliver(s, mates):
        q = offset(s)
        for e in mates:
            for r in range(2):
                at = jnp.clip(place_ref[r, q * PLANE + e], 0, caps[s] - 1)
                packet = moved[s][at]
                if e == 0:
                    out_ref[q, r] = packet
                else:
                    staged[s, e, (e + r) % 2] = packet
        for e in mates:
            if e:
                spread(s, e).start()

    low, high = range(PLANE // 2), range(PLANE // 2, PLANE)
    for s in range(half):
        for c, (first, last) in enumerate(spans(caps[s])):
            hop(s, c).wait_recv()
            if s + 1 < half and first < caps[s + 1]:
                hop(s + 1, c).start()
        if s + 1 < half:
            deliver(s, range(PLANE))
        else:

            @pl.when(w == 0)
            def _():
                deliver(half - 1, low)

            @pl.when(w == 1)
            def _():
                deliver(half - 1, high)

    for s in range(half):
        for c in range(len(spans(caps[s]))):
            hop(s, c).wait_send()
    for e in range(1, PLANE):
        visit(e).wait()
        for s in range(half - 1):
            spread(s, e).wait_send()

    @pl.when(w == 0)
    def _():
        for e in low:
            if e:
                spread(half - 1, e).wait_send()

    @pl.when(w == 1)
    def _():
        for e in high:
            spread(half - 1, e).wait_send()

    def arrival(q, chip):
        return pltpu.make_async_remote_copy(
            src_ref=staged.at[0, 1],
            dst_ref=out_ref.at[q, pl.ds(2 * chip, 2)],
            send_sem=send_x.at[0, 1],
            recv_sem=recv_x.at[q, chip],
            device_id=partner(z * PLANE + mate(j, 1)),
            device_id_type=MESH,
        )

    for q in range(1, planes):
        for chip in range(1, 4):
            arrival(q, chip).wait_recv()

    @pl.when(w == 1)
    def _():
        for q in range(1, half + 1):
            arrival(q, 0).wait_recv()

    @pl.when(w == 0)
    def _():
        for q in range(half + 1, planes):
            arrival(q, 0).wait_recv()


def carry(planes, caps, number, lists, count, moment, onset, slip, green):
    size = planes * PLANE
    half = planes // 2
    chunks = len(spans(caps[0]))
    before = before_table(planes)
    reach, limit = reach_tables(planes, caps)
    vmem = pl.BlockSpec(memory_space=pltpu.VMEM)
    smem = pl.BlockSpec(memory_space=pltpu.SMEM)
    hbm = pl.BlockSpec(memory_space=pl.ANY)
    packet = (64, 128)
    dma = pltpu.SemaphoreType.DMA
    return pl.pallas_call(
        functools.partial(carry_kernel, planes, caps),
        out_shape=(
            jax.ShapeDtypeStruct((planes, PLANE, *packet), jnp.int16),
            jax.ShapeDtypeStruct((1, 1), jnp.int32),
            jax.ShapeDtypeStruct(onset.shape, jnp.int32),
            jax.ShapeDtypeStruct(onset.shape, jnp.int32),
            jax.ShapeDtypeStruct(slip.shape, jnp.float32),
        ),
        in_specs=[vmem, smem, vmem, vmem, vmem, vmem, vmem, vmem, hbm],
        out_specs=(vmem,) * 5,
        scratch_shapes=[
            pltpu.VMEM((1, 1, 128), jnp.float32),
            pltpu.VMEM((size, 1, 128), jnp.float32),
            pltpu.VMEM((8, 2 * size), jnp.float32),
            pltpu.VMEM((1, 2 * size), jnp.int32),
            pltpu.VMEM((8, size), jnp.int32),
            pltpu.SMEM((8, 2 * size), jnp.float32),
            pltpu.SMEM((1, 2 * size), jnp.int32),
            pltpu.SMEM((8, size), jnp.int32),
            pltpu.VMEM((2 * green.shape[0], *green.shape[1:]), green.dtype),
            pltpu.VMEM((caps[0], *packet), jnp.int16),
            pltpu.VMEM((half, PLANE, 2, *packet), jnp.int16),
            pltpu.VMEM((PLANE, *packet), jnp.int16),
            *[pltpu.VMEM((caps[s], *packet), jnp.int16) for s in range(half)],
            dma((PLANE,)),
            dma((PLANE,)),
            dma((planes,)),
            dma((planes,)),
            dma,
            dma,
            dma,
            dma((3,)),
            dma((half, chunks)),
            dma((half, chunks)),
            dma((half, PLANE)),
            dma((planes, 4)),
            dma((PLANE,)),
            dma((PLANE,)),
        ],
        compiler_params=pltpu.CompilerParams(
            collective_id=number, has_side_effects=True, vmem_limit_bytes=VMEM_LIMIT
        ),
        name="carry",
    )(
        lists, count, moment, onset, slip, jnp.asarray(before, jnp.bfloat16),
        jnp.asarray(reach, jnp.bfloat16), jnp.asarray(limit), green,
    )


def halves(value):
    coarse = value.astype(jnp.bfloat16)
    return coarse, (value - coarse.astype(jnp.float32)).astype(jnp.bfloat16)


def motion_kernel(
    planes, list_ref, count_ref, start_ref, rest_ref, slip_ref, moment_ref, packet_ref, rate_ref, out_ref,
    wide, motion,
):
    me = lax.axis_index("pts")
    z, j = me // PLANE, me % PLANE
    variations = out_ref.shape[0]
    bound = jnp.abs(moment_ref[0, 0])
    for s in range(1, 6):
        bound = bound + jnp.abs(moment_ref[0, s])
    lane = lax.broadcasted_iota(jnp.int32, (16, 128), 1)
    motion[...] = jnp.zeros_like(motion)
    wide[...] = jnp.zeros_like(wide)
    count = count_ref[0]

    def add_blocks(pair, carry):
        for n in range(2):
            k = 2 * pair + n
            holder = list_ref[0, k] // BLOCKS
            q = (z - holder // PLANE + planes) % planes
            e = j ^ (holder % PLANE)
            unit = jnp.where(k < count, bound, 0.0) * (LIMIT / TOP**4)
            for p in range(4):
                code = packet_ref[q, e, pl.ds(16 * p, 16), :].astype(jnp.int32).astype(jnp.float32)
                square = code * jnp.abs(code)
                trace = square * jnp.abs(square) * unit
                wide[4 * n + p, 0, pl.ds(8, 16), :] = trace
                wide[4 * n + p, 1, pl.ds(10, 16), :] = trace
        for v in range(variations):
            total = None
            for i in range(8):
                start = start_ref[pair, v * 8 + i]
                rest = rest_ref[pair, v * 8 + i]
                trace = jnp.where(
                    lane + rest < 128, wide[i, 0, pl.ds(start, 16), :], wide[i, 1, pl.ds(start, 16), :]
                )
                term = slip_ref[pair, v * 8 + i] * pltpu.roll(trace, rest, 1)
                total = term if total is None else total + term
            motion[v, pl.ds(8, 16), :] += total
        return carry

    lax.fori_loop(0, (count + 1) // 2, add_blocks, 0)

    row = lax.broadcasted_iota(jnp.int32, (128, 128), 0)
    column = lax.broadcasted_iota(jnp.int32, (128, 128), 1)
    for v in range(variations):
        rate = jnp.broadcast_to(rate_ref[pl.ds(v, 1), :], (128, 128))
        rate = pltpu.roll(rate, 0, 1, stride=1, stride_axis=0)
        taps = jnp.concatenate(
            [jnp.where(column >= row, rate, 0.0), jnp.where(column < row, rate, 0.0)], axis=0
        )
        signal = jnp.concatenate([motion[v, pl.ds(8, 16), :], motion[v, pl.ds(6, 16), :]], axis=1)
        coarse, fine = halves(signal)
        taps, rest = halves(taps)
        both = jnp.dot(
            jnp.concatenate([coarse, fine], axis=0), taps, preferred_element_type=jnp.float32
        )
        out_ref[v] = (
            both[:16] + both[16:] + jnp.dot(coarse, rest, preferred_element_type=jnp.float32)
        )


def synthesize(planes, block_list, count, start, rest, slip, moment, packets, rate):
    variations = slip.shape[0]
    smem = pl.BlockSpec(memory_space=pltpu.SMEM)
    vmem = pl.BlockSpec(memory_space=pltpu.VMEM)
    return pl.pallas_call(
        functools.partial(motion_kernel, planes),
        out_shape=jax.ShapeDtypeStruct((variations, 16, 128), jnp.float32),
        in_specs=[smem, smem, smem, smem, smem, smem, vmem, vmem],
        out_specs=vmem,
        scratch_shapes=[
            pltpu.VMEM((8, 2, 32, 128), jnp.float32),
            pltpu.VMEM((variations, 24, 128), jnp.float32),
        ],
        compiler_params=pltpu.CompilerParams(vmem_limit_bytes=VMEM_LIMIT),
        name="synthesize",
    )(block_list, count, start, rest, slip, moment, packets, rate)


CAPS = (36, 33, 29, 26, 22, 18, 13, 8)


def local(planes, green_tensors, block_lists, block_count, onset_steps, slip_amount, mechanism, slip_rate):
    held, points, strains, parts, length = green_tensors.shape
    green = green_tensors.reshape(held, points, strains, parts, length // 128, 128)
    green = green.transpose(0, 1, 2, 4, 3, 5).reshape(held, points, strains, -1, 128)
    asked = (block_lists, block_count, mechanism, onset_steps[0], slip_amount[0], green)
    packets, over, start, rest, weight = carry(planes, CAPS, 0, *asked)

    def finish(arrived):
        seis = synthesize(
            planes, block_lists, block_count, start, rest, weight, mechanism, arrived, slip_rate[0]
        )
        seis = seis.reshape(-1, length // 128, parts, 128).transpose(0, 2, 1, 3)
        return seis.reshape(1, -1, parts, length)

    return lax.cond(
        over[0, 0] > 0,
        lambda arrived: finish(carry(planes, most_packets(planes), 1, *asked)[0]),
        finish,
        packets,
    )


def solution(mesh):
    planes = mesh.shape["pts"] // PLANE
    placed = tuple(P(SITE_PTS, *[None] * n) for n in (4, 1, 0, 2, 2, 1, 2))
    return jax.shard_map(
        functools.partial(local, planes),
        mesh=mesh,
        in_specs=placed,
        out_specs=P(SITE_PTS, None, None, None),
        check_vma=False,
    )
```

```python
import functools

import jax
import jax.numpy as jnp
import numpy as np
from jax import lax
from jax.experimental import pallas as pl
from jax.experimental.pallas import tpu as pltpu
from jax.sharding import PartitionSpec as P

MESH = pl.DeviceIdType.MESH
HIGHEST = lax.Precision.HIGHEST
SITE_PTS = ("site", "pts")
PLANE = 8
LIMIT = 6.0
TOP = 32767.0
CHUNK = 4
BLOCKS = 16
VMEM_LIMIT = 60 * 1024 * 1024


def mate(j, e):
    for bit in (1, 2, 4):
        if e & bit:
            j = j + bit * (1 - 2 * ((j // bit) % 2))
    return j


def partner(index):
    return {"pts": index}


def train_of(planes):
    half = planes // 2
    dz = np.arange(planes * PLANE) // PLANE
    e = np.arange(planes * PLANE) % PLANE
    up = ((dz >= 1) & (dz < half)) | ((dz == half) & (e < PLANE // 2))
    down = (dz > half) | ((dz == half) & (e >= PLANE // 2))
    distance = np.where(up, dz, np.where(down, planes - dz, 0))
    return distance, up.astype(np.int32) - down.astype(np.int32), e


def before_table(planes):
    distance, way, e = train_of(planes)
    same = (way[:, None] == way[None, :]) & (way[:, None] != 0)
    ahead = (distance[:, None] > distance[None, :]) | (
        (distance[:, None] == distance[None, :]) & (e[:, None] < e[None, :])
    )
    return (same & ahead).astype(np.float32)


def reach_tables(planes, caps):
    distance, way, e = train_of(planes)
    half = planes // 2
    size = planes * PLANE
    reach = np.zeros((size, size), np.float32)
    limit = np.full((4 * planes, size), 1e6, np.float32)
    for chip in range(4):
        turned = np.arange(size) ^ (2 * chip)
        for s in range(1, half + 1):
            for w, sign in enumerate((1, -1)):
                column = chip * planes + w * half + s - 1
                reach[:, column] = ((way == sign) & (distance >= s))[turned]
                limit[chip * planes : (chip + 1) * planes, column] = caps[s - 1]
    return reach, limit


def most_packets(planes):
    half = planes // 2
    return tuple(2 * (PLANE * (half - s) + PLANE // 2) for s in range(1, half + 1))


def turn_blocks(value):
    rows, size = value.shape
    skewed = pltpu.roll(value, 0, 1, stride=8, stride_axis=0)
    row = lax.broadcasted_iota(jnp.int32, value.shape, 0)
    block = lax.broadcasted_iota(jnp.int32, value.shape, 1) // 8
    turned = jnp.zeros_like(value)
    for n in range(rows):
        picked = jnp.where(block == ((row + n) & (rows - 1)), skewed, 0.0)
        picked = jnp.sum(picked, axis=0, keepdims=True)
        if n:
            picked = pltpu.roll(picked, size - 8 * n, 1)
        turned = jnp.where(row == n, picked, turned)
    return turned


def spans(count):
    return [(first, min(first + CHUNK, count)) for first in range(0, count, CHUNK)]


def carry_kernel(
    planes, caps, list_in, count_ref, moment_in, onset_in, slip_in, before_in, reach_in,
    limit_in, green_ref, out_ref, over_ref, start_ref, rest_ref, weight_ref, *scratch,
):
    half = planes // 2
    (row_ref, rows_ref, tab_made, block_made, place_made, tab_ref, block_ref, place_ref) = scratch[:8]
    list_ref, moment_ref, onset_ref, slip_ref, before_ref, reach_ref, limit_ref = scratch[8:15]
    green, own, staged, near = scratch[15:19]
    moved = scratch[19 : 19 + half]
    (
        send_a, recv_a, send_b, recv_b, send_g, recv_g, load_sem, table_sem,
        send_z, recv_z, send_x, recv_x, send_n, recv_n, fetch_sem,
    ) = scratch[19 + half :]
    me = lax.axis_index("pts")
    z, j = me // PLANE, me % PLANE
    size = planes * PLANE
    listed = list_in.shape[1]
    strains = moment_in.shape[1]

    fetches = [
        pltpu.make_async_copy(kept, here, fetch_sem.at[n])
        for n, (kept, here) in enumerate(
            (
                (list_in, list_ref), (moment_in, moment_ref), (onset_in, onset_ref),
                (slip_in, slip_ref), (before_in, before_ref), (reach_in, reach_ref),
                (limit_in, limit_ref),
            )
        )
    ]
    for copy in fetches:
        copy.start()
    barrier = pltpu.get_barrier_semaphore()
    for e in range(1, PLANE):
        pl.semaphore_signal(
            barrier, inc=1, device_id=partner(z * PLANE + mate(j, e)), device_id_type=MESH
        )
    for d in range(1, planes):
        pl.semaphore_signal(
            barrier, inc=1, device_id=partner(((z + d) % planes) * PLANE + j), device_id_type=MESH
        )
    load = pltpu.make_async_copy(green_ref, green.at[pl.ds(0, BLOCKS)], load_sem)
    load.start()
    for copy in fetches:
        copy.wait()
    entry = lax.broadcasted_iota(jnp.int32, (1, listed), 1)
    names = jnp.where(entry < count_ref[0], list_ref[...], -1).astype(jnp.float32)
    row_ref[...] = jnp.zeros_like(row_ref)
    row_ref[0, :, pl.ds(0, listed)] = names
    row_ref[0, :, pl.ds(listed + 1, strains)] = moment_ref[...]
    rows_ref[pl.ds(0, 1)] = row_ref[...]
    pl.semaphore_wait(barrier, PLANE - 1 + planes - 1)

    copies = []
    for e in range(1, PLANE):
        copies.append(
            pltpu.make_async_remote_copy(
                src_ref=row_ref,
                dst_ref=rows_ref.at[pl.ds(e, 1)],
                send_sem=send_a.at[e],
                recv_sem=recv_a.at[e],
                device_id=partner(z * PLANE + mate(j, e)),
                device_id_type=MESH,
            )
        )
    for copy in copies:
        copy.start()
    other = pltpu.make_async_remote_copy(
        src_ref=green_ref,
        dst_ref=green.at[pl.ds(BLOCKS, BLOCKS)],
        send_sem=send_g,
        recv_sem=recv_g,
        device_id=partner(z * PLANE + mate(j, 1)),
        device_id_type=MESH,
    )
    other.start()
    for copy in copies:
        copy.wait()
    copies = []
    for d in range(1, planes):
        copies.append(
            pltpu.make_async_remote_copy(
                src_ref=rows_ref.at[pl.ds(0, PLANE)],
                dst_ref=rows_ref.at[pl.ds((planes - d) * PLANE, PLANE)],
                send_sem=send_b.at[d],
                recv_sem=recv_b.at[d],
                device_id=partner(((z + d) % planes) * PLANE + j),
                device_id_type=MESH,
            )
        )
    for copy in copies:
        copy.start()
    onset = turn_blocks(onset_ref[...].astype(jnp.float32)).astype(jnp.int32)
    start_ref[...] = 8 - 2 * (onset >> 7)
    rest_ref[...] = onset & 127
    weight_ref[...] = turn_blocks(slip_ref[...])
    for copy in copies:
        copy.wait()

    turned = rows_ref[...].reshape(size, 128).T
    named = turned[:listed]
    holder = jnp.floor(named * (1.0 / BLOCKS))
    source = lax.broadcasted_iota(jnp.int32, (size, size), 0)
    lane = lax.broadcasted_iota(jnp.int32, (size, size), 1)
    at = (z + planes - (source & (planes - 1))) & (planes - 1)
    source_id = (at * PLANE + (j ^ (source // planes))).astype(jnp.float32)
    active = jnp.zeros((size, size), jnp.float32)
    for k in range(listed):
        active = active + jnp.where(holder[k : k + 1, :] == source_id, 1.0, 0.0)
    view = pltpu.roll(active, 0, 1, stride=PLANE, stride_axis=0)
    chips = jnp.concatenate(
        [
            view[2 * g * planes : (2 * g + 1) * planes] + view[(2 * g + 1) * planes : (2 * g + 2) * planes]
            for g in range(4)
        ],
        axis=0,
    ).astype(jnp.bfloat16)
    counts = jnp.dot(chips, reach_ref[...], preferred_element_type=jnp.float32)
    excess = jnp.max(counts - limit_ref[...], axis=0, keepdims=True)
    excess = jnp.max(excess, axis=1, keepdims=True)
    over_ref[...] = jnp.where(excess > 0.5, 1, 0).astype(jnp.int32)

    first = jnp.dot(chips[:planes], before_ref[...], preferred_element_type=jnp.float32)
    second = first + view[:planes]
    diagonal = (lane[:planes] // PLANE) == source[:planes]
    part = lax.broadcasted_iota(jnp.int32, (8, size), 0)
    place = jnp.where(
        part == 0,
        jnp.sum(jnp.where(diagonal, first, 0.0), axis=0, keepdims=True),
        jnp.sum(jnp.where(diagonal, second, 0.0), axis=0, keepdims=True),
    )
    place_made[...] = place.astype(jnp.int32)

    moment = turned[32:40]
    bound = LIMIT * jnp.sum(
        jnp.where((part >= 1) & (part <= strains), jnp.abs(moment), 0.0), axis=0, keepdims=True
    )
    gain = 1.0 / jnp.maximum(bound, 1e-30)
    moment = jnp.where(part == 7, gain, moment)
    side = lane[:1]
    way = jnp.where(side < PLANE, 0, jnp.where(side < (planes // 2) * PLANE + PLANE // 2, 1, -1))
    mine = way == 1 - 2 * (j % 2)
    slot = source.astype(jnp.float32)

    def info(owner, shift):
        owner = owner.astype(jnp.float32)
        block = jnp.where(holder == owner, named - (BLOCKS * owner - shift), 0.0)
        return jnp.where(part == 0, jnp.sum(block, axis=0, keepdims=True), moment)

    def table(which, held, position):
        chosen = (held > 0.5) & mine & (position == slot)
        return lax.dot_general(
            which,
            jnp.where(chosen, 1.0, 0.0),
            (((1,), (1,)), ((), ())),
            precision=HIGHEST,
            preferred_element_type=jnp.float32,
        )

    own_info = info(me, 0.0)
    both = table(own_info, view[:1], first[:1]) + table(
        info(me + 1 - 2 * (j % 2), float(BLOCKS)), view[planes : planes + 1], second[:1]
    )
    tab_made[:, :size] = both
    tab_made[:, size:] = own_info
    block_made[:, :size] = both[:1].astype(jnp.int32)
    block_made[:, size:] = own_info[:1].astype(jnp.int32)
    tables = [
        pltpu.make_async_copy(made, held, table_sem.at[n])
        for n, (made, held) in enumerate(
            ((tab_made, tab_ref), (block_made, block_ref), (place_made, place_ref))
        )
    ]
    for copy in tables:
        copy.start()
    other.wait()
    load.wait()
    for copy in tables:
        copy.wait()

    w = j % 2

    def trace(entry, write):
        block = jnp.clip(block_ref[0, entry], 0, 2 * BLOCKS - 1)
        moment = [tab_ref[1 + s, entry] for s in range(6)]
        gain = tab_ref[7, entry]
        for p in range(4):
            total = moment[0] * green[block, p, 0].astype(jnp.float32)
            for s in range(1, 6):
                total = total + moment[s] * green[block, p, s].astype(jnp.float32)
            root = lax.rsqrt(lax.rsqrt(jnp.abs(total) * gain))
            level = jnp.minimum(root * TOP, TOP)
            code = jnp.round(jnp.where(total < 0.0, -level, level)).astype(jnp.int32)
            write(p, code.astype(jnp.int16))

    def hop(s, c):
        first, last = spans(caps[s])[c]
        source = own if s == 0 else moved[s - 1]
        return pltpu.make_async_remote_copy(
            src_ref=source.at[pl.ds(first, last - first)],
            dst_ref=moved[s].at[pl.ds(first, last - first)],
            send_sem=send_z.at[s, c],
            recv_sem=recv_z.at[s, c],
            device_id=partner(((z + 1 + w * (planes - 2)) % planes) * PLANE + j),
            device_id_type=MESH,
        )

    def offset(s):
        return (s + 1) + w * (planes - 2 * (s + 1))

    def spread(s, e):
        return pltpu.make_async_remote_copy(
            src_ref=staged.at[s, e],
            dst_ref=out_ref.at[offset(s), pl.ds(e - e % 2, 2)],
            send_sem=send_x.at[s, e],
            recv_sem=recv_x.at[offset(s), e // 2],
            device_id=partner(z * PLANE + mate(j, e)),
            device_id_type=MESH,
        )

    def visit(e):
        return pltpu.make_async_remote_copy(
            src_ref=near.at[e],
            dst_ref=out_ref.at[0, e],
            send_sem=send_n.at[e],
            recv_sem=recv_n.at[e],
            device_id=partner(z * PLANE + mate(j, e)),
            device_id_type=MESH,
        )

    for c, (first, last) in enumerate(spans(caps[0])):

        def fill(i, carry):
            def write(p, code):
                own[i, pl.ds(16 * p, 16), :] = code

            trace(i, write)
            return carry

        lax.fori_loop(first, last, fill, 0)
        hop(0, c).start()

    def write_own(p, code):
        out_ref[0, 0, pl.ds(16 * p, 16), :] = code

    trace(size, write_own)

    def fill_near(e, carry):
        def write(p, code):
            near[e, pl.ds(16 * p, 16), :] = code

        trace(size + e, write)
        return carry

    lax.fori_loop(1, PLANE, fill_near, 0)
    for e in range(1, PLANE):
        visit(e).start()

    def deliver(s, mates):
        q = offset(s)
        for e in mates:
            for r in range(2):
                at = jnp.clip(place_ref[r, q * PLANE + e], 0, caps[s] - 1)
                packet = moved[s][at]
                if e == 0:
                    out_ref[q, r] = packet
                else:
                    staged[s, e, (e + r) % 2] = packet
        for e in mates:
            if e:
                spread(s, e).start()

    low, high = range(PLANE // 2), range(PLANE // 2, PLANE)
    for s in range(half):
        for c, (first, last) in enumerate(spans(caps[s])):
            hop(s, c).wait_recv()
            if s + 1 < half and first < caps[s + 1]:
                hop(s + 1, c).start()
        if s + 1 < half:
            deliver(s, range(PLANE))
        else:

            @pl.when(w == 0)
            def _():
                deliver(half - 1, low)

            @pl.when(w == 1)
            def _():
                deliver(half - 1, high)

    for s in range(half):
        for c in range(len(spans(caps[s]))):
            hop(s, c).wait_send()
    for e in range(1, PLANE):
        visit(e).wait()
        for s in range(half - 1):
            spread(s, e).wait_send()

    @pl.when(w == 0)
    def _():
        for e in low:
            if e:
                spread(half - 1, e).wait_send()

    @pl.when(w == 1)
    def _():
        for e in high:
            spread(half - 1, e).wait_send()

    def arrival(q, chip):
        return pltpu.make_async_remote_copy(
            src_ref=staged.at[0, 1],
            dst_ref=out_ref.at[q, pl.ds(2 * chip, 2)],
            send_sem=send_x.at[0, 1],
            recv_sem=recv_x.at[q, chip],
            device_id=partner(z * PLANE + mate(j, 1)),
            device_id_type=MESH,
        )

    for q in range(1, planes):
        for chip in range(1, 4):
            arrival(q, chip).wait_recv()

    @pl.when(w == 1)
    def _():
        for q in range(1, half + 1):
            arrival(q, 0).wait_recv()

    @pl.when(w == 0)
    def _():
        for q in range(half + 1, planes):
            arrival(q, 0).wait_recv()


def carry(planes, caps, number, lists, count, moment, onset, slip, green):
    size = planes * PLANE
    half = planes // 2
    chunks = len(spans(caps[0]))
    before = before_table(planes)
    reach, limit = reach_tables(planes, caps)
    vmem = pl.BlockSpec(memory_space=pltpu.VMEM)
    smem = pl.BlockSpec(memory_space=pltpu.SMEM)
    hbm = pl.BlockSpec(memory_space=pl.ANY)
    packet = (64, 128)
    dma = pltpu.SemaphoreType.DMA
    return pl.pallas_call(
        functools.partial(carry_kernel, planes, caps),
        out_shape=(
            jax.ShapeDtypeStruct((planes, PLANE, *packet), jnp.int16),
            jax.ShapeDtypeStruct((1, 1), jnp.int32),
            jax.ShapeDtypeStruct(onset.shape, jnp.int32),
            jax.ShapeDtypeStruct(onset.shape, jnp.int32),
            jax.ShapeDtypeStruct(slip.shape, jnp.float32),
        ),
        in_specs=[hbm, smem, hbm, hbm, hbm, hbm, hbm, hbm, hbm],
        out_specs=(vmem,) * 5,
        scratch_shapes=[
            pltpu.VMEM((1, 1, 128), jnp.float32),
            pltpu.VMEM((size, 1, 128), jnp.float32),
            pltpu.VMEM((8, 2 * size), jnp.float32),
            pltpu.VMEM((1, 2 * size), jnp.int32),
            pltpu.VMEM((8, size), jnp.int32),
            pltpu.SMEM((8, 2 * size), jnp.float32),
            pltpu.SMEM((1, 2 * size), jnp.int32),
            pltpu.SMEM((8, size), jnp.int32),
            pltpu.VMEM(lists.shape, jnp.int32),
            pltpu.VMEM(moment.shape, jnp.float32),
            pltpu.VMEM(onset.shape, jnp.int32),
            pltpu.VMEM(slip.shape, jnp.float32),
            pltpu.VMEM(before.shape, jnp.bfloat16),
            pltpu.VMEM(reach.shape, jnp.bfloat16),
            pltpu.VMEM(limit.shape, jnp.float32),
            pltpu.VMEM((2 * green.shape[0], *green.shape[1:]), green.dtype),
            pltpu.VMEM((caps[0], *packet), jnp.int16),
            pltpu.VMEM((half, PLANE, 2, *packet), jnp.int16),
            pltpu.VMEM((PLANE, *packet), jnp.int16),
            *[pltpu.VMEM((caps[s], *packet), jnp.int16) for s in range(half)],
            dma((PLANE,)),
            dma((PLANE,)),
            dma((planes,)),
            dma((planes,)),
            dma,
            dma,
            dma,
            dma((3,)),
            dma((half, chunks)),
            dma((half, chunks)),
            dma((half, PLANE)),
            dma((planes, 4)),
            dma((PLANE,)),
            dma((PLANE,)),
            dma((7,)),
        ],
        compiler_params=pltpu.CompilerParams(
            collective_id=number, has_side_effects=True, vmem_limit_bytes=VMEM_LIMIT
        ),
        name="carry",
    )(
        lists, count, moment, onset, slip, jnp.asarray(before, jnp.bfloat16),
        jnp.asarray(reach, jnp.bfloat16), jnp.asarray(limit), green,
    )


def halves(value):
    coarse = value.astype(jnp.bfloat16)
    return coarse, (value - coarse.astype(jnp.float32)).astype(jnp.bfloat16)


def motion_kernel(
    planes, list_ref, count_ref, start_ref, rest_ref, slip_ref, moment_ref, packet_ref, rate_ref, out_ref,
    wide, motion,
):
    me = lax.axis_index("pts")
    z, j = me // PLANE, me % PLANE
    variations = out_ref.shape[0]
    bound = jnp.abs(moment_ref[0, 0])
    for s in range(1, 6):
        bound = bound + jnp.abs(moment_ref[0, s])
    lane = lax.broadcasted_iota(jnp.int32, (16, 128), 1)
    motion[...] = jnp.zeros_like(motion)
    wide[...] = jnp.zeros_like(wide)
    count = count_ref[0]

    def add_blocks(turn, carry):
        for n in range(4):
            k = 4 * turn + n
            holder = list_ref[0, k] // BLOCKS
            q = (z - holder // PLANE + planes) % planes
            e = j ^ (holder % PLANE)
            unit = jnp.where(k < count, bound, 0.0) * (LIMIT / TOP**4)
            for p in range(4):
                code = packet_ref[q, e, pl.ds(16 * p, 16), :].astype(jnp.int32).astype(jnp.float32)
                square = code * jnp.abs(code)
                trace = square * jnp.abs(square) * unit
                wide[4 * n + p, 0, pl.ds(8, 16), :] = trace
                wide[4 * n + p, 1, pl.ds(10, 16), :] = trace
        for v in range(variations):
            total = None
            for i in range(16):
                pair, at = 2 * turn + i // 8, v * 8 + i % 8
                start = start_ref[pair, at]
                rest = rest_ref[pair, at]
                trace = jnp.where(
                    lane + rest < 128, wide[i, 0, pl.ds(start, 16), :], wide[i, 1, pl.ds(start, 16), :]
                )
                term = slip_ref[pair, at] * pltpu.roll(trace, rest, 1)
                total = term if total is None else total + term
            motion[v, pl.ds(8, 16), :] += total
        return carry

    lax.fori_loop(0, (count + 3) // 4, add_blocks, 0)

    row = lax.broadcasted_iota(jnp.int32, (128, 128), 0)
    column = lax.broadcasted_iota(jnp.int32, (128, 128), 1)
    for v in range(variations):
        rate = jnp.broadcast_to(rate_ref[pl.ds(v, 1), :], (128, 128))
        rate = pltpu.roll(rate, 0, 1, stride=1, stride_axis=0)
        taps = jnp.concatenate(
            [jnp.where(column >= row, rate, 0.0), jnp.where(column < row, rate, 0.0)], axis=0
        )
        signal = jnp.concatenate([motion[v, pl.ds(8, 16), :], motion[v, pl.ds(6, 16), :]], axis=1)
        coarse, fine = halves(signal)
        taps, rest = halves(taps)
        both = jnp.dot(
            jnp.concatenate([coarse, fine], axis=0), taps, preferred_element_type=jnp.float32
        )
        out_ref[v] = (
            both[:16] + both[16:] + jnp.dot(coarse, rest, preferred_element_type=jnp.float32)
        )


def synthesize(planes, block_list, count, start, rest, slip, moment, packets, rate):
    variations = slip.shape[0]
    smem = pl.BlockSpec(memory_space=pltpu.SMEM)
    vmem = pl.BlockSpec(memory_space=pltpu.VMEM)
    return pl.pallas_call(
        functools.partial(motion_kernel, planes),
        out_shape=jax.ShapeDtypeStruct((variations, 16, 128), jnp.float32),
        in_specs=[smem, smem, smem, smem, smem, smem, vmem, vmem],
        out_specs=vmem,
        scratch_shapes=[
            pltpu.VMEM((16, 2, 32, 128), jnp.float32),
            pltpu.VMEM((variations, 24, 128), jnp.float32),
        ],
        compiler_params=pltpu.CompilerParams(vmem_limit_bytes=VMEM_LIMIT),
        name="synthesize",
    )(block_list, count, start, rest, slip, moment, packets, rate)


CAPS = (36, 33, 29, 26, 22, 18, 13, 8)


def local(planes, green_tensors, block_lists, block_count, onset_steps, slip_amount, mechanism, slip_rate):
    held, points, strains, parts, length = green_tensors.shape
    green = green_tensors.reshape(held, points, strains, parts, length // 128, 128)
    green = green.transpose(0, 1, 2, 4, 3, 5).reshape(held, points, strains, -1, 128)
    asked = (block_lists, block_count, mechanism, onset_steps[0], slip_amount[0], green)
    packets, over, start, rest, weight = carry(planes, CAPS, 0, *asked)

    def finish(arrived):
        seis = synthesize(
            planes, block_lists, block_count, start, rest, weight, mechanism, arrived, slip_rate[0]
        )
        seis = seis.reshape(-1, length // 128, parts, 128).transpose(0, 2, 1, 3)
        return seis.reshape(1, -1, parts, length)

    return lax.cond(
        over[0, 0] > 0,
        lambda arrived: finish(carry(planes, most_packets(planes), 1, *asked)[0]),
        finish,
        packets,
    )


def solution(mesh):
    planes = mesh.shape["pts"] // PLANE
    placed = tuple(P(SITE_PTS, *[None] * n) for n in (4, 1, 0, 2, 2, 1, 2))
    return jax.shard_map(
        functools.partial(local, planes),
        mesh=mesh,
        in_specs=placed,
        out_specs=P(SITE_PTS, None, None, None),
        check_vma=False,
    )
```
